32 devices in a mesh: dp: 16 (over z, x, core), mp: 2 (over y).
Axes of the slice: x: 2, y: 2, z: 4, core: 2. Of those that a mesh axis runs over, the one named last changes fastest.
Arguments:
- inputs_store: bfloat16 [512, 128], replicated, may hold values from -6 to 6
- window: int32 [16], replicated, may hold values from 0 to 511
- targets_store: bfloat16 [512, 4096], P(None, ('dp', 'mp')), may hold values from -6 to 6
- jac_store: bfloat16 [512, 4096, 128], P(None, ('dp', 'mp')), may hold values from -4 to 4
- first_weight: bfloat16 [128, 1024], replicated, may hold values from -0.5 to 0.5
- first_bias: bfloat16 [1024], replicated, may hold values from -3 to 3
- hidden_weight: bfloat16 [1024, 1024], P(None, 'mp'), may hold values from -0.1875 to 0.1875
- hidden_bias: bfloat16 [1024], P('mp'), may hold values from -3 to 3
- decoder_weight: bfloat16 [4096, 1024], P(('dp', 'mp')), may hold values from -0.1875 to 0.1875
Outputs:
- first_weights: float32 [128, 1024], replicated
- first_biases: float32 [1024], replicated
- hidden_weights: float32 [1024, 1024], P(None, 'mp')
- hidden_biases: float32 [1024], P('mp')
- decoder_grad: float32 [4096, 1024], P(('dp', 'mp'))
The draws below stay inside these ranges and needn't reach their ends.
Inputs may be any that keep to these rules, and one draw needn't show every extreme that they name: `window`: indices of stored samples; an index may repeat.
All inputs are finite; a program needn't handle non-finite values.
Results may differ from the reference program's by a relative error of at most 0.011.
Values may be sent and summed in bfloat16 or wider, within the bound.
No kernel may reach another device: no remote copies, remote signals or barrier semaphores. Data moves between devices by JAX's collectives and lax.ppermute only.
A program may use at most 64 MiB of HBM per device.

```python
import math
import jax
import jax.numpy as jnp
from jax import lax

RANK = 128
H = 1024
OUT = 4096
NSTORE = 512
SAMPLES = 16
N_DP = 16
N_MP = 2


def place_ends(values, stream_key, low, high):
    dims = values.shape
    place = [jax.random.randint(jax.random.fold_in(stream_key, axis), (), 0, dims[axis]) for axis in range(len(dims))]
    values = values.at[tuple(place)].set(low)
    longest = dims.index(max(dims))
    place[longest] = (place[longest] + 1) % dims[longest]
    return values.at[tuple(place)].set(high)


def steps_of(key, shape, pieces, low, top_value):
    loudness = 1.0
    for axis_at, blocks in pieces:
        steps = jax.random.uniform(jax.random.fold_in(jax.random.fold_in(key, 6), axis_at), (blocks,), jnp.float32, low / len(pieces), top_value / len(pieces))
        loudness = loudness * jnp.repeat(jnp.exp(steps), shape[axis_at] // blocks).reshape((-1,) + (1,) * (len(shape) - 1 - axis_at))
    return loudness


def centred(key, extent, scale, most, pieces=(), kind=jnp.bfloat16):
    factor_of = steps_of(key, extent, pieces, -0.22, 0.18) if pieces else 1.0
    values = jax.random.normal(key, extent, jnp.float32) * scale * factor_of
    return jnp.minimum(jnp.maximum(values, -most), most).astype(kind)


def setup_inputs(seed: int = 0) -> dict:
    keys = jax.random.split(jax.random.key(seed), 10)
    return {
        "inputs_store": centred(keys[0], (NSTORE, RANK), 1.0, 6.0),
        "window": place_ends(jax.random.randint(keys[1], (SAMPLES,), 0, NSTORE), jax.random.fold_in(keys[1], 1), 0, NSTORE - 1).astype(jnp.int32),
        "targets_store": centred(keys[2], (NSTORE, OUT), 1.0, 6.0, ((1, 32),)),
        "jac_store": centred(keys[3], (NSTORE, OUT, RANK), 0.3, 4.0, ((1, 32),)),
        "first_weight": centred(keys[4], (RANK, H), RANK ** -0.5, 0.5),
        "first_bias": centred(keys[5], (H,), 0.5, 3.0),
        "hidden_weight": centred(keys[6], (H, H), H ** -0.5, 0.1875, ((1, 2),)),
        "hidden_bias": centred(keys[7], (H,), 0.5, 3.0, ((0, 2),)),
        "decoder_weight": centred(keys[8], (OUT, H), H ** -0.5, 0.1875, ((0, 32),)),
    }


def rounded(values):
    return lax.optimization_barrier(values.astype(jnp.bfloat16)).astype(jnp.float32)


def reference(inputs_store, window, targets_store, jac_store, first_weight, first_bias, hidden_weight, hidden_bias, decoder_weight):
    block = math.gcd(SAMPLES, 8)
    out_rows = OUT // (N_DP * N_MP)
    weight_one = first_weight.astype(jnp.float32)
    weight_two = hidden_weight.astype(jnp.float32)
    readout_weight = decoder_weight.astype(jnp.float32)
    dec_groups = readout_weight.reshape(N_DP, N_MP, out_rows, H)

    def block_step(totals, indices):
        grad_one, bias_one, grad_two, bias_two, decoder_gradient = totals
        inputs = inputs_store[indices]
        targets = targets_store[indices].astype(jnp.float32)
        jacobians = jac_store[indices].astype(jnp.float32)
        first_pre = jnp.dot(inputs, first_weight, preferred_element_type=jnp.float32) + first_bias.astype(jnp.float32)
        first_act = jnp.tanh(first_pre)
        first_slope = 1.0 - first_act * first_act
        first_tan = rounded(first_slope[:, None, :] * weight_one[None])
        first_round = rounded(first_act)
        hidden_lin = jnp.einsum("srh,hk->srk", first_tan, weight_two)
        hidden_pre = jnp.einsum("sh,hk->sk", first_round, weight_two) + hidden_bias.astype(jnp.float32)
        hidden_act = jnp.tanh(hidden_pre)
        hidden_slope = 1.0 - hidden_act * hidden_act
        hidden_tangent = rounded(hidden_slope[:, None, :] * hidden_lin)
        hidden_rounded_state = rounded(hidden_act)
        outputs_net = jnp.einsum("sk,ok->so", hidden_rounded_state, readout_weight)
        jacobian_predicted = jnp.einsum("mvn,an->mav", hidden_tangent, readout_weight)
        output_residual = rounded(outputs_net - targets)
        jacobian_residual = rounded(jacobian_predicted - jacobians)
        decoder_gradient = decoder_gradient + jnp.einsum("qi,qm->im", output_residual, hidden_rounded_state) + jnp.einsum("hzy,hym->zm", jacobian_residual, hidden_tangent)
        miss_groups = output_residual.reshape(block, N_DP, N_MP, out_rows)
        jac_groups = jacobian_residual.reshape(block, N_DP, N_MP, out_rows, RANK)
        act_back = jnp.sum(rounded(jnp.einsum("sdmk,dmkh->smh", miss_groups, dec_groups)), axis=1)
        tan_back = jnp.sum(rounded(jnp.einsum("sdmkr,dmkh->smrh", jac_groups, dec_groups)), axis=1)
        lin_back = tan_back * hidden_slope[:, None, :]
        pre_back = act_back * hidden_slope - 2.0 * hidden_act * hidden_slope * jnp.sum(tan_back * hidden_lin, axis=1)
        lin_round = rounded(lin_back)
        pre_round = rounded(pre_back)
        grad_two = grad_two + jnp.einsum("sh,sk->hk", first_round, pre_round) + jnp.einsum("srh,srk->hk", first_tan, lin_round)
        bias_two = bias_two + jnp.sum(pre_back, axis=0)
        tan_lower = jnp.einsum("srk,hk->srh", lin_round, weight_two)
        act_lower = jnp.einsum("sk,hk->sh", pre_round, weight_two)
        pre_lower = act_lower * first_slope - 2.0 * first_act * first_slope * jnp.sum(tan_lower * weight_one[None], axis=1)
        grad_one = grad_one + jnp.einsum("sr,sh->rh", inputs.astype(jnp.float32), pre_lower, precision=lax.Precision.HIGHEST) + jnp.sum(tan_lower * first_slope[:, None, :], axis=0)
        bias_one = bias_one + jnp.sum(pre_lower, axis=0)
        return (grad_one, bias_one, grad_two, bias_two, decoder_gradient), None

    start_totals = (jnp.zeros((RANK, H), jnp.float32), jnp.zeros((H,), jnp.float32), jnp.zeros((H, H), jnp.float32), jnp.zeros((H,), jnp.float32), jnp.zeros((OUT, H), jnp.float32))
    totals, unused = lax.scan(block_step, start_totals, window.reshape(-1, block))
    return totals[0], totals[1], totals[2], totals[3], totals[4]
```

```python
import jax
import jax.numpy as jnp
from jax import lax
from jax.sharding import Mesh, PartitionSpec as P

F32 = jnp.float32
BF16 = jnp.bfloat16


def dot(a, b, contract):
    return lax.dot_general(a, b, (contract, ((), ())), preferred_element_type=F32)


def swap(value, axes, size, step):
    return lax.ppermute(value, axes, [(j, j ^ step) for j in range(size)])


def tree_sum(parts):
    while len(parts) > 1:
        parts = [parts[i] + parts[i + 1] for i in range(0, len(parts), 2)]
    return parts[0]


def place(pieces, me, axis):
    width = pieces[0].shape[axis]
    shape = list(pieces[0].shape)
    shape[axis] *= len(pieces)
    whole = jnp.zeros(shape, pieces[0].dtype)
    for step, piece in enumerate(pieces):
        whole = lax.dynamic_update_slice_in_dim(whole, piece, (me ^ step) * width, axis)
    return whole


def part(value, index, count, axis):
    width = value.shape[axis] // count
    return lax.dynamic_slice_in_dim(value, index * width, width, axis)


def make_step(nz, nx, nc, ny):
    nxy = nx * ny

    def on_device(
        inputs_store,
        window,
        targets_store,
        jac_store,
        first_weight,
        first_bias,
        hidden_weight,
        hidden_bias,
        decoder_weight,
    ):
        z, x, c, y = (lax.axis_index(name) for name in ("z", "x", "c", "y"))
        xy = x * ny + y
        rank, hidden = first_weight.shape
        kw = hidden_weight.shape[1]
        pieces = [hidden_weight]
        biases = [hidden_bias]
        mine = part(hidden_weight, c, nc, 0)
        for t in range(1, ny):
            got = swap(mine, "y", ny, t)
            rest = [got] + [swap(got, "c", nc, u) for u in range(1, nc)]
            pieces.append(place(rest, c, 0))
            biases.append(swap(hidden_bias, "y", ny, t))
        wide_hidden = jnp.concatenate(pieces, axis=1)
        wide_bias = jnp.concatenate(biases)
        jac_parts, target_parts, decoder_parts = [], [], []
        for u in range(nc):
            rows = part(window, c ^ u, nc, 0)
            jac, target = jac_store[rows], targets_store[rows]
            decoder = decoder_weight
            if u:
                jac, target, decoder = (swap(v, "c", nc, u) for v in (jac, target, decoder))
            jac_parts.append(jac)
            target_parts.append(target)
            decoder_parts.append(decoder)
        jac = jnp.concatenate(jac_parts, axis=1)
        target = jnp.concatenate(target_parts, axis=1)
        decoder = jnp.concatenate(decoder_parts, axis=0)
        decoder = jnp.concatenate([part(decoder, y ^ t, ny, 1) for t in range(ny)], axis=1)
        inputs = inputs_store[part(window, c, nc, 0)]
        count = inputs.shape[0]
        weight_one = first_weight.astype(F32)
        first_act = jnp.tanh(dot(inputs, first_weight, ((1,), (0,))) + first_bias.astype(F32))
        first_slope = 1.0 - first_act * first_act
        first_tan = (first_slope[:, None, :] * weight_one[None]).astype(BF16)
        first_tan = first_tan.reshape(count * rank, hidden)
        first_round = first_act.astype(BF16)
        hidden_lin = dot(first_tan, wide_hidden, ((1,), (0,))).reshape(count, rank, -1)
        hidden_act = jnp.tanh(
            dot(first_round, wide_hidden, ((1,), (0,))) + wide_bias.astype(F32)
        )
        hidden_slope = 1.0 - hidden_act * hidden_act
        hidden_tan = (hidden_slope[:, None, :] * hidden_lin).astype(BF16)
        hidden_round = hidden_act.astype(BF16)
        output_miss = dot(hidden_round, decoder, ((1,), (1,))) - target.astype(F32)
        output_miss = output_miss.astype(BF16)
        jac_net = dot(decoder, hidden_tan, ((1,), (2,)))
        jac_miss = (jac_net - jac.transpose(1, 0, 2).astype(F32)).astype(BF16)
        jac_miss = jac_miss.reshape(-1, count * rank)
        grad = dot(output_miss, hidden_round, ((0,), (0,))) + dot(
            jac_miss, hidden_tan.reshape(count * rank, -1), ((1,), (0,))
        )
        blocks = jnp.split(grad, nc, axis=0)
        own = [blocks[0]] + [swap(blocks[u], "c", nc, u) for u in range(1, nc)]
        grad = tree_sum(own)
        decoder_grad = place(jnp.split(grad, ny, axis=1), y, 1)

        act_back = dot(output_miss, decoder, ((1,), (0,)))
        tan_back = dot(jac_miss, decoder, ((0,), (0,))).reshape(count, rank, -1)
        pre_back = act_back * hidden_slope - 2.0 * hidden_act * hidden_slope * jnp.sum(
            tan_back * hidden_lin, axis=1
        )
        lin_round = (tan_back * hidden_slope[:, None, :]).astype(BF16)
        lin_round = lin_round.reshape(count * rank, -1)
        pre_round = pre_back.astype(BF16)
        hidden_grad = dot(first_round, pre_round, ((0,), (0,))) + dot(
            first_tan, lin_round, ((0,), (0,))
        )
        tan_lower = dot(lin_round, wide_hidden, ((1,), (1,))).reshape(count, rank, hidden)
        act_lower = dot(pre_round, wide_hidden, ((1,), (1,)))
        pre_lower = act_lower * first_slope - 2.0 * first_act * first_slope * jnp.sum(
            tan_lower * weight_one[None], axis=1
        )
        first_grad = jnp.einsum(
            "sr,sh->rh", inputs.astype(F32), pre_lower, precision=lax.Precision.HIGHEST
        ) + jnp.sum(tan_lower * first_slope[:, None, :], axis=0)
        hidden_bsum = jnp.sum(pre_back, axis=0).reshape(ny, kw)
        hidden_bsum = place([hidden_bsum[t : t + 1] for t in range(ny)], y, 0)
        first_bsum = jnp.sum(pre_lower, axis=0).reshape(ny, kw)
        bias_sum = jnp.concatenate([hidden_bsum, first_bsum])

        def exchange(axes, size, hidden_of, first_of, bias):
            totals = []
            for s in range(size):
                sent = (hidden_of(s), first_of(s), bias)
                sent = [v.astype(BF16) for v in sent]
                if s:
                    sent = [swap(v, axes, size, s) for v in sent]
                totals.append([v.astype(F32) for v in sent])
            return [tree_sum(list(group)) for group in zip(*totals)]

        hidden_grad, first_grad, bias_sum = exchange(
            "c",
            nc,
            lambda s: part(hidden_grad, c ^ s, nc, 0),
            lambda s: part(first_grad, c ^ s, nc, 0),
            bias_sum,
        )
        whole_hidden, whole_first = hidden_grad, first_grad
        hidden_grad, first_grad, bias_sum = exchange(
            ("x", "y"),
            nxy,
            lambda s: part(whole_hidden, x ^ (s // ny), nx, 0)[
                :, (s % ny) * kw : (s % ny + 1) * kw
            ],
            lambda s: part(part(whole_first, x ^ (s // ny), nx, 0), y ^ (s % ny), ny, 1),
            bias_sum,
        )
        half_hidden, half_first = hidden_grad, first_grad
        hidden_grad, first_grad, bias_sum = exchange(
            "z",
            nz,
            lambda s: part(half_hidden, z ^ s, nz, 0),
            lambda s: part(half_first, z ^ s, nz, 0),
            bias_sum,
        )

        def spread(value, axes, size, me, axis):
            return place([value] + [swap(value, axes, size, s) for s in range(1, size)], me, axis)

        hidden_out = hidden_grad.astype(BF16)
        first_out = first_grad.astype(BF16)
        hidden_out = spread(hidden_out, "z", nz, z, 0)
        first_out = spread(first_out, "z", nz, z, 0)
        hidden_out = spread(hidden_out, "x", nx, x, 0)
        first_out = spread(first_out, "x", nx, x, 0)
        first_out = spread(first_out, "y", ny, y, 1)
        hidden_out = spread(hidden_out, "c", nc, c, 0)
        first_out = spread(first_out, "c", nc, c, 0)
        return (
            first_out.astype(F32),
            bias_sum[ny:].reshape(-1),
            hidden_out.astype(F32),
            bias_sum[y],
            decoder_grad,
        )

    return on_device


def solution(mesh):
    dp, mp = mesh.shape["dp"], mesh.shape["mp"]
    nc = 2 if dp % 2 == 0 else 1
    nx = 2 if dp % (2 * nc) == 0 else 1
    nz = dp // (nc * nx)
    fine = Mesh(mesh.devices.reshape(nz, nx, nc, mp), ("z", "x", "c", "y"))
    dps = ("z", "x", "c")
    every = dps + ("y",)
    placed = (
        P(),
        P(),
        P(None, every),
        P(None, every, None),
        P(),
        P(),
        P(None, "y"),
        P("y"),
        P(every, None),
    )
    return jax.shard_map(
        make_step(nz, nx, nc, mp),
        mesh=fine,
        in_specs=placed,
        out_specs=(P(), P(), P(None, "y"), P("y"), P(every, None)),
        check_vma=False,
    )
```

```python
import jax
import jax.numpy as jnp
from jax import lax
from jax.experimental import pallas as pl
from jax.experimental.pallas import tpu as pltpu
from jax.sharding import Mesh, PartitionSpec as P

F32 = jnp.float32
BF16 = jnp.bfloat16


def dot(a, b, contract):
    return lax.dot_general(a, b, (contract, ((), ())), preferred_element_type=F32)


def swap(value, axes, size, step):
    return lax.ppermute(value, axes, [(j, j ^ step) for j in range(size)])


def tree_sum(parts):
    while len(parts) > 1:
        parts = [parts[i] + parts[i + 1] for i in range(0, len(parts), 2)]
    return parts[0]


def place(pieces, me, axis):
    width = pieces[0].shape[axis]
    shape = list(pieces[0].shape)
    shape[axis] *= len(pieces)
    whole = jnp.zeros(shape, pieces[0].dtype)
    for step, piece in enumerate(pieces):
        whole = lax.dynamic_update_slice_in_dim(whole, piece, (me ^ step) * width, axis)
    return whole


def part(value, index, count, axis):
    width = value.shape[axis] // count
    return lax.dynamic_slice_in_dim(value, index * width, width, axis)


VMEM = pl.BlockSpec(memory_space=pltpu.VMEM)
SMEM = pl.BlockSpec(memory_space=pltpu.SMEM)
ANY = pl.BlockSpec(memory_space=pltpu.HBM)


COST_UNIT = 1 << 30


def aligned(index, size):
    return pl.ds(pl.multiple_of(index * size, size), size)


def local_call(body, outs, args, name, specs=None, scratch=(), limit=24 << 20, cost=1.0):
    return pl.pallas_call(
        body,
        out_shape=[jax.ShapeDtypeStruct(shape, kind) for shape, kind in outs],
        in_specs=[VMEM] * len(args) if specs is None else specs,
        out_specs=[VMEM] * len(outs),
        scratch_shapes=list(scratch),
        compiler_params=pltpu.CompilerParams(vmem_limit_bytes=limit),
        cost_estimate=pl.CostEstimate(
            flops=int(cost * COST_UNIT), bytes_accessed=1 << 20, transcendentals=0
        ),
        name=name,
    )(*args)


def make_fast_step(nz, nx, nc, ny):
    nxy = nx * ny

    def on_device(
        inputs_store,
        window,
        targets_store,
        jac_store,
        first_weight,
        first_bias,
        hidden_weight,
        hidden_bias,
        decoder_weight,
    ):
        rank, hidden = first_weight.shape
        kw = hidden_weight.shape[1]
        outs, depth = decoder_weight.shape[0], inputs_store.shape[0]
        count = window.shape[0] // nc
        total = (count + 1) * rank
        hrow_c, frow_c = hidden // nc, rank // nc
        hrow_x, frow_x = hrow_c // nx, frow_c // nx
        hrow_z, frow_z = hrow_x // nz, frow_x // nz
        brow = 16

        def cut(weight_ref, out_ref, sems):
            me = lax.axis_index("c")
            size = hrow_c // 8
            copies = [
                pltpu.make_async_copy(
                    weight_ref.at[aligned(me * 8 + i, size)],
                    out_ref.at[pl.ds(i * size, size)],
                    sems.at[i],
                )
                for i in range(8)
            ]
            for copy in copies:
                copy.start()
            for copy in copies:
                copy.wait()

        (sent,) = local_call(
            cut,
            [((hrow_c, kw), BF16)],
            (hidden_weight,),
            "cut",
            cost=2,
            specs=[ANY],
            scratch=[pltpu.SemaphoreType.DMA((8,))],
            limit=60 << 20,
        )
        got = swap(sent, "y", ny, 1)
        bias_got = swap(hidden_bias, "y", ny, 1)
        decoder_got = swap(decoder_weight, "c", nc, 1)

        def gather(
            window_ref, jac_ref, target_ref, input_ref, weight_ref, bias_ref,
            own_ref, away_ref, act_ref, turned_ref, sems,
        ):
            me = lax.axis_index("c")
            copies = []
            for u, ref in enumerate((away_ref, own_ref)):
                for i in range(count):
                    row = window_ref[(me ^ u ^ 1) * count + i]
                    copies.append(pltpu.make_async_copy(jac_ref.at[row], ref.at[i], sems.at[u, i]))
            for copy in copies:
                copy.start()
            line = lax.broadcasted_iota(jnp.int32, (rank, depth), 0)
            place_of = lax.broadcasted_iota(jnp.int32, (rank, depth), 1)

            def pick(member, table):
                index = jnp.full((rank, depth), -1, jnp.int32)
                for i in range(count):
                    index = jnp.where(line == i, window_ref[member * count + i], index)
                chosen = jnp.where(index == place_of, 1.0, 0.0).astype(BF16)
                return jnp.dot(chosen, table, preferred_element_type=F32)

            inputs = pick(me, input_ref[...])
            turned_ref[...] = inputs.T
            first_pre = jnp.dot(
                inputs.astype(BF16), weight_ref[...], preferred_element_type=F32
            )[:count]
            act_ref[...] = jnp.tanh(first_pre + bias_ref[...].astype(F32).reshape(1, hidden))
            own_ref[count] = pick(me, target_ref[...]).T.astype(BF16)
            away_ref[count] = pick(me ^ 1, target_ref[...]).T.astype(BF16)
            for copy in copies:
                copy.wait()

        jac_shape = ((count + 1,) + jac_store.shape[1:], BF16)
        jac_own, jac_away, first_act, turned = local_call(
            gather,
            [jac_shape, jac_shape, ((count, hidden), F32), ((rank, rank), F32)],
            (window, jac_store, targets_store, inputs_store, first_weight, first_bias),
            "gather",
            cost=4,
            specs=[SMEM, ANY, VMEM, VMEM, VMEM, VMEM],
            scratch=[pltpu.SemaphoreType.DMA((nc, count))],
            limit=60 << 20,
        )
        jac_got = swap(jac_away, "c", nc, 1)

        def warm(act_ref, weight_ref, half_ref, tan_ref, side_ref, lin_ref):
            act = act_ref[...]
            slope = 1.0 - act * act
            weight = weight_ref[...].astype(F32)
            pad = jnp.zeros((rank - count, hidden), F32)
            for s in range(count):
                rows = slice(s * rank, (s + 1) * rank)
                tan_ref[rows] = (slope[s : s + 1] * weight).astype(BF16)
            padded = jnp.concatenate([act, pad])
            tan_ref[count * rank :] = padded.astype(BF16)
            lin_ref[...] = jnp.dot(tan_ref[...], half_ref[...], preferred_element_type=F32)
            slope_side = jnp.concatenate([slope, pad]).T
            weight_side = weight.T
            for s in range(count):
                columns = slice(s * rank, (s + 1) * rank)
                side_ref[:, columns] = (slope_side[:, s : s + 1] * weight_side).astype(BF16)
            side_ref[:, count * rank :] = padded.T.astype(BF16)

        first_tan, first_side, lin_own = local_call(
            warm,
            [((total, hidden), BF16), ((hidden, total), BF16), ((total, kw), F32)],
            (first_act, first_weight, hidden_weight),
            "warm",
            cost=2,
            limit=30 << 20,
        )
        got, bias_got, decoder_got, jac_got, first_tan = lax.optimization_barrier(
            (got, bias_got, decoder_got, jac_got, first_tan)
        )
        got_core = swap(got, "c", nc, 1)

        def main(
            tan1_ref, side_ref, lin_ref, got_ref, core_ref, bias_ref, bias_got_ref,
            dec_ref, dec_got_ref, jac_ref, jac_got_ref,
            half_ref, tan_ref, miss_ref, round_ref, sum_ref, out_ref,
            lin_got_ref, wide_ref, net_ref, back_ref,
        ):
            me, my = lax.axis_index("c"), lax.axis_index("y")
            half_ref[aligned(me, hrow_c)] = got_ref[...]
            half_ref[aligned(me ^ 1, hrow_c)] = core_ref[...]
            for b in range(ny):
                columns = slice(b * kw, (b + 1) * kw)
                wide_ref[:outs, columns] = dec_ref[:, aligned(my ^ b, kw)]
                wide_ref[outs:, columns] = dec_got_ref[:, aligned(my ^ b, kw)]
            lin_got_ref[...] = jnp.dot(tan1_ref[...], half_ref[...], preferred_element_type=F32)
            pad = jnp.zeros((rank - count, kw), F32)
            last = slice(count * rank, total)
            lins, acts, slopes = (lin_ref, lin_got_ref), [], []
            for b, (lin, bias) in enumerate(zip(lins, (bias_ref, bias_got_ref))):
                columns = slice(b * kw, (b + 1) * kw)
                pre = lin[count * rank : count * rank + count]
                act = jnp.tanh(pre + bias[...].astype(F32).reshape(1, kw))
                slope = 1.0 - act * act
                acts.append(act)
                slopes.append(slope)
                tan_ref[last, columns] = jnp.concatenate([act, pad]).astype(BF16)
                for s in range(count):
                    rows = slice(s * rank, (s + 1) * rank)
                    tan_ref[rows, columns] = (slope[s : s + 1] * lin[rows]).astype(BF16)
            net_ref[...] = dot(wide_ref[...], tan_ref[...], ((1,), (1,)))
            for s in range(count + 1):
                columns = slice(s * rank, (s + 1) * rank)
                for part_rows, jac in ((slice(0, outs), jac_ref), (slice(outs, None), jac_got_ref)):
                    miss = net_ref[part_rows, columns] - jac[s].astype(F32)
                    miss_ref[part_rows, columns] = miss.astype(BF16)
            back_ref[...] = dot(miss_ref[...], wide_ref[...], ((0,), (0,)))
            for b, lin in enumerate(lins):
                columns = slice(b * kw, (b + 1) * kw)
                act, slope = acts[b], slopes[b]
                sums = []
                for s in range(count):
                    rows = slice(s * rank, (s + 1) * rank)
                    back = back_ref[rows, columns]
                    sums.append(jnp.sum(back * lin[rows], axis=0, keepdims=True))
                    round_ref[rows, columns] = (back * slope[s : s + 1]).astype(BF16)
                act_back = back_ref[count * rank : count * rank + count, columns]
                sums = jnp.concatenate(sums)
                pre_back = act_back * slope - 2.0 * act * slope * sums
                round_ref[last, columns] = jnp.concatenate([pre_back, pad]).astype(BF16)
                sum_ref[:, columns] = jnp.sum(pre_back, axis=0, keepdims=True)
            out_ref[...] = jnp.dot(
                side_ref[aligned(me ^ 1, hrow_c)], round_ref[...], preferred_element_type=F32
            ).astype(BF16)

        half_got, hidden_tan, miss, lin_round, hidden_sum, g_away = local_call(
            main,
            [
                ((hidden, kw), BF16),
                ((total, hidden), BF16),
                ((nc * outs, total), BF16),
                ((total, hidden), BF16),
                ((1, hidden), F32),
                ((hrow_c, hidden), BF16),
            ],
            (
                first_tan, first_side, lin_own, got, got_core, hidden_bias, bias_got,
                decoder_weight, decoder_got, jac_own, jac_got,
            ),
            "main",
            cost=6.5,
            scratch=[
                pltpu.VMEM((total, kw), F32),
                pltpu.VMEM((nc * outs, hidden), BF16),
                pltpu.VMEM((nc * outs, total), F32),
                pltpu.VMEM((total, hidden), F32),
            ],
            limit=40 << 20,
        )
        g_got = swap(g_away, "c", nc, 1)

        def lower(
            round_ref, half_ref, got_ref, act_ref, weight_ref, turned_ref, sum_ref,
            own_ref, away_ref, bias_ref, low_ref, first_ref,
        ):
            me, my = lax.axis_index("c"), lax.axis_index("y")
            low_ref[...] = dot(round_ref[:, :kw], half_ref[...], ((1,), (1,)))
            low_ref[...] += dot(round_ref[:, kw:], got_ref[...], ((1,), (1,)))
            act = act_ref[...]
            slope = 1.0 - act * act
            weight = weight_ref[...].astype(F32)
            sums = []
            for s in range(count):
                low = low_ref[s * rank : (s + 1) * rank]
                sums.append(jnp.sum(low * weight, axis=0, keepdims=True))
            act_lower = low_ref[count * rank : count * rank + count]
            pre_lower = act_lower * slope - 2.0 * act * slope * jnp.concatenate(sums)
            turned = turned_ref[...]
            value = jnp.zeros((rank, hidden), F32)
            for s in range(count):
                low = low_ref[s * rank : (s + 1) * rank]
                value = value + low * slope[s : s + 1]
                value = value + turned[:, s : s + 1] * pre_lower[s : s + 1]
            first_ref[...] = value
            own_ref[...] = first_ref[aligned(me, frow_c)]
            for b in range(ny):
                away = first_ref[aligned(me ^ 1, frow_c), b * kw : (b + 1) * kw]
                away_ref[b * frow_c : (b + 1) * frow_c] = away.astype(BF16)
            sums = sum_ref[...]
            halves = [sums[:, :kw], sums[:, kw:]]
            first_sum = jnp.sum(pre_lower, axis=0, keepdims=True)
            bias = jnp.concatenate(
                [
                    jnp.where(my == 0, halves[0], halves[1]),
                    jnp.where(my == 0, halves[1], halves[0]),
                    first_sum[:, :kw],
                    first_sum[:, kw:],
                    jnp.zeros((brow - 2 * ny, kw), F32),
                ]
            ).astype(BF16)
            away_ref[ny * frow_c :] = bias
            bias_ref[...] = bias

        f_own, f_away, b_own = local_call(
            lower,
            [
                ((frow_c, hidden), F32),
                ((ny * frow_c + brow, kw), BF16),
                ((brow, kw), BF16),
            ],
            (lin_round, hidden_weight, half_got, first_act, first_weight, turned, hidden_sum),
            "lower",
            cost=3,
            scratch=[pltpu.VMEM((total, hidden), F32), pltpu.VMEM((rank, hidden), F32)],
            limit=30 << 20,
        )
        f_got = swap(f_away, "c", nc, 1)

        def own_rows(side_ref, round_ref, out_ref):
            me = lax.axis_index("c")
            out_ref[...] = jnp.dot(
                side_ref[aligned(me, hrow_c)], round_ref[...], preferred_element_type=F32
            )

        (g_own,) = local_call(
            own_rows, [((hrow_c, hidden), F32)], (first_side, lin_round), "own_rows", cost=1.5, limit=16 << 20
        )

        def merge_core(g_ref, gg_ref, f_ref, fg_ref, b_ref, *out_refs):
            mx, my = lax.axis_index("x"), lax.axis_index("y")
            bias = b_ref[...].astype(F32) + fg_ref[ny * frow_c :].astype(F32)
            for s, out_ref in enumerate(out_refs):
                a, b = s // ny, s % ny
                rows = aligned(mx ^ a, hrow_x)
                columns = slice(b * kw, (b + 1) * kw)
                value = g_ref[rows, columns] + gg_ref[rows, columns].astype(F32)
                out_ref[:hrow_x] = value.astype(BF16)
                rows, columns = aligned(mx ^ a, frow_x), aligned(my ^ b, kw)
                from_core = pl.ds(
                    pl.multiple_of((my ^ b) * frow_c + (mx ^ a) * frow_x, frow_x), frow_x
                )
                value = f_ref[rows, columns] + fg_ref[from_core].astype(F32)
                out_ref[hrow_x : hrow_x + frow_x] = value.astype(BF16)
                out_ref[hrow_x + frow_x :] = bias.astype(BF16)

        plane = local_call(
            merge_core,
            [((hrow_x + frow_x + brow, kw), BF16)] * nxy,
            (g_own, g_got, f_own, f_got, b_own),
            "merge_core",
        )
        (miss, hidden_tan), _ = lax.optimization_barrier(((miss, hidden_tan), plane[0]))
        plane = [plane[0]] + [swap(plane[s], ("x", "y"), nxy, s) for s in range(1, nxy)]

        def readout(miss_ref, tan_ref, own_ref, away_ref):
            own_ref[...] = jnp.dot(miss_ref[:outs], tan_ref[...], preferred_element_type=F32)
            away_ref[...] = jnp.dot(miss_ref[outs:], tan_ref[...], preferred_element_type=F32)

        d_own, d_away = local_call(
            readout, [((outs, hidden), F32)] * 2, (miss, hidden_tan), "readout", cost=1, limit=16 << 20
        )
        *plane, d_away = lax.optimization_barrier((*plane, d_away))
        d_got = swap(d_away, "c", nc, 1)

        def join(own_ref, got_ref, out_ref):
            my = lax.axis_index("y")
            for b in range(ny):
                columns = slice(b * kw, (b + 1) * kw)
                out_ref[:, aligned(my ^ b, kw)] = own_ref[:, columns] + got_ref[:, columns]

        (decoder_grad,) = local_call(
            join, [((outs, hidden), F32)], (d_own, d_got), "join", cost=1, limit=8 << 20
        )

        def merge_plane(*refs):
            in_refs, out_refs, total = refs[:nxy], refs[nxy:-1], refs[-1]
            mz = lax.axis_index("z")
            total[...] = tree_sum([ref[...].astype(F32) for ref in in_refs])
            for s, out_ref in enumerate(out_refs):
                out_ref[:hrow_z] = total[aligned(mz ^ s, hrow_z)].astype(BF16)
                out_ref[hrow_z : hrow_z + brow] = total[hrow_x + frow_x :].astype(BF16)
                rows = pl.ds(pl.multiple_of(hrow_x + (mz ^ s) * frow_z, frow_z), frow_z)
                out_ref[hrow_z + brow :] = total[rows].astype(BF16)

        line = local_call(
            merge_plane,
            [((hrow_z + brow + frow_z, kw), BF16)] * nz,
            tuple(plane),
            "merge_plane",
            scratch=[pltpu.VMEM((hrow_x + frow_x + brow, kw), F32)],
        )
        line = [line[0]] + [swap(line[s], "z", nz, s) for s in range(1, nz)]

        *line, decoder_grad = lax.optimization_barrier((*line, decoder_grad))

        def merge_line(*refs):
            in_refs, (out_ref, hidden_ref, first_ref) = refs[:nz], refs[nz:]
            my = lax.axis_index("y")
            total = tree_sum([ref[...].astype(F32) for ref in in_refs])
            out_ref[:hrow_z] = total[:hrow_z].astype(BF16)
            out_ref[hrow_z:] = total[hrow_z + brow :].astype(BF16)
            bias = total[hrow_z : hrow_z + brow]
            hidden_ref[...] = jnp.where(my == 0, bias[0:1], bias[1:2]).reshape(kw)
            for b in range(ny):
                row = bias[ny + b : ny + b + 1]
                first_ref[b * kw : (b + 1) * kw] = row.reshape(kw)

        piece, hidden_bias_out, first_bias_out = local_call(
            merge_line,
            [((hrow_z + frow_z, kw), BF16), ((kw,), F32), ((hidden,), F32)],
            tuple(line),
            "merge_line",
        )
        pieces = [piece] + [swap(piece, "z", nz, s) for s in range(1, nz)]

        def stack_line(*refs):
            in_refs, (out_ref, first_ref) = refs[:nz], refs[nz:]
            mz = lax.axis_index("z")
            for s, ref in enumerate(in_refs):
                out_ref[mz ^ s] = ref[...]
                first_ref[mz ^ s] = ref[hrow_z:]

        both, first = local_call(
            stack_line,
            [((nz, hrow_z + frow_z, kw), BF16), ((nz, frow_z, kw), BF16)],
            tuple(pieces),
            "stack_line",
        )
        held = [
            swap(both if s % ny == 0 else first, ("x", "y"), nxy, s) if s else both
            for s in range(nxy)
        ]
        held = list(lax.optimization_barrier(tuple(held)))
        held += [swap(value, "c", nc, 1) for value in held]

        def spread_out(*refs):
            in_refs, (hidden_ref, first_ref) = refs[: nc * nxy], refs[nc * nxy :]
            mx, mc, my = lax.axis_index("x"), lax.axis_index("c"), lax.axis_index("y")
            for s, ref in enumerate(in_refs):
                u, a, b = s // nxy, s % nxy // ny, s % ny
                base = (mc ^ u) * nx + (mx ^ a)
                for i in range(nz):
                    value = ref[i].astype(F32)
                    if b == 0:
                        hidden_ref[aligned(base * nz + i, hrow_z)] = value[:hrow_z]
                        value = value[hrow_z:]
                    first_ref[aligned(base * nz + i, frow_z), aligned(my ^ b, kw)] = value

        hidden_out, first_out = local_call(
            spread_out,
            [((hidden, kw), F32), ((rank, hidden), F32)],
            tuple(held),
            "spread_out",
            cost=2,
        )
        return (
            first_out,
            first_bias_out,
            hidden_out,
            hidden_bias_out,
            decoder_grad,
        )

    return on_device


def make_step(nz, nx, nc, ny):
    nxy = nx * ny

    def on_device(
        inputs_store,
        window,
        targets_store,
        jac_store,
        first_weight,
        first_bias,
        hidden_weight,
        hidden_bias,
        decoder_weight,
    ):
        z, x, c, y = (lax.axis_index(name) for name in ("z", "x", "c", "y"))
        xy = x * ny + y
        rank, hidden = first_weight.shape
        kw = hidden_weight.shape[1]
        pieces = [hidden_weight]
        biases = [hidden_bias]
        mine = part(hidden_weight, c, nc, 0)
        for t in range(1, ny):
            got = swap(mine, "y", ny, t)
            rest = [got] + [swap(got, "c", nc, u) for u in range(1, nc)]
            pieces.append(place(rest, c, 0))
            biases.append(swap(hidden_bias, "y", ny, t))
        wide_hidden = jnp.concatenate(pieces, axis=1)
        wide_bias = jnp.concatenate(biases)
        jac_parts, target_parts, decoder_parts = [], [], []
        for u in range(nc):
            rows = part(window, c ^ u, nc, 0)
            jac, target = jac_store[rows], targets_store[rows]
            decoder = decoder_weight
            if u:
                jac, target, decoder = (swap(v, "c", nc, u) for v in (jac, target, decoder))
            jac_parts.append(jac)
            target_parts.append(target)
            decoder_parts.append(decoder)
        jac = jnp.concatenate(jac_parts, axis=1)
        target = jnp.concatenate(target_parts, axis=1)
        decoder = jnp.concatenate(decoder_parts, axis=0)
        decoder = jnp.concatenate([part(decoder, y ^ t, ny, 1) for t in range(ny)], axis=1)
        inputs = inputs_store[part(window, c, nc, 0)]
        count = inputs.shape[0]
        weight_one = first_weight.astype(F32)
        first_act = jnp.tanh(dot(inputs, first_weight, ((1,), (0,))) + first_bias.astype(F32))
        first_slope = 1.0 - first_act * first_act
        first_tan = (first_slope[:, None, :] * weight_one[None]).astype(BF16)
        first_tan = first_tan.reshape(count * rank, hidden)
        first_round = first_act.astype(BF16)
        hidden_lin = dot(first_tan, wide_hidden, ((1,), (0,))).reshape(count, rank, -1)
        hidden_act = jnp.tanh(
            dot(first_round, wide_hidden, ((1,), (0,))) + wide_bias.astype(F32)
        )
        hidden_slope = 1.0 - hidden_act * hidden_act
        hidden_tan = (hidden_slope[:, None, :] * hidden_lin).astype(BF16)
        hidden_round = hidden_act.astype(BF16)
        output_miss = dot(hidden_round, decoder, ((1,), (1,))) - target.astype(F32)
        output_miss = output_miss.astype(BF16)
        jac_net = dot(decoder, hidden_tan, ((1,), (2,)))
        jac_miss = (jac_net - jac.transpose(1, 0, 2).astype(F32)).astype(BF16)
        jac_miss = jac_miss.reshape(-1, count * rank)
        grad = dot(output_miss, hidden_round, ((0,), (0,))) + dot(
            jac_miss, hidden_tan.reshape(count * rank, -1), ((1,), (0,))
        )
        blocks = jnp.split(grad, nc, axis=0)
        own = [blocks[0]] + [swap(blocks[u], "c", nc, u) for u in range(1, nc)]
        grad = tree_sum(own)
        decoder_grad = place(jnp.split(grad, ny, axis=1), y, 1)

        act_back = dot(output_miss, decoder, ((1,), (0,)))
        tan_back = dot(jac_miss, decoder, ((0,), (0,))).reshape(count, rank, -1)
        pre_back = act_back * hidden_slope - 2.0 * hidden_act * hidden_slope * jnp.sum(
            tan_back * hidden_lin, axis=1
        )
        lin_round = (tan_back * hidden_slope[:, None, :]).astype(BF16)
        lin_round = lin_round.reshape(count * rank, -1)
        pre_round = pre_back.astype(BF16)
        hidden_grad = dot(first_round, pre_round, ((0,), (0,))) + dot(
            first_tan, lin_round, ((0,), (0,))
        )
        tan_lower = dot(lin_round, wide_hidden, ((1,), (1,))).reshape(count, rank, hidden)
        act_lower = dot(pre_round, wide_hidden, ((1,), (1,)))
        pre_lower = act_lower * first_slope - 2.0 * first_act * first_slope * jnp.sum(
            tan_lower * weight_one[None], axis=1
        )
        first_grad = jnp.einsum(
            "sr,sh->rh", inputs.astype(F32), pre_lower, precision=lax.Precision.HIGHEST
        ) + jnp.sum(tan_lower * first_slope[:, None, :], axis=0)
        hidden_bsum = jnp.sum(pre_back, axis=0).reshape(ny, kw)
        hidden_bsum = place([hidden_bsum[t : t + 1] for t in range(ny)], y, 0)
        first_bsum = jnp.sum(pre_lower, axis=0).reshape(ny, kw)
        bias_sum = jnp.concatenate([hidden_bsum, first_bsum])

        def exchange(axes, size, hidden_of, first_of, bias):
            totals = []
            for s in range(size):
                sent = (hidden_of(s), first_of(s), bias)
                sent = [v.astype(BF16) for v in sent]
                if s:
                    sent = [swap(v, axes, size, s) for v in sent]
                totals.append([v.astype(F32) for v in sent])
            return [tree_sum(list(group)) for group in zip(*totals)]

        hidden_grad, first_grad, bias_sum = exchange(
            "c",
            nc,
            lambda s: part(hidden_grad, c ^ s, nc, 0),
            lambda s: part(first_grad, c ^ s, nc, 0),
            bias_sum,
        )
        whole_hidden, whole_first = hidden_grad, first_grad
        hidden_grad, first_grad, bias_sum = exchange(
            ("x", "y"),
            nxy,
            lambda s: part(whole_hidden, x ^ (s // ny), nx, 0)[
                :, (s % ny) * kw : (s % ny + 1) * kw
            ],
            lambda s: part(part(whole_first, x ^ (s // ny), nx, 0), y ^ (s % ny), ny, 1),
            bias_sum,
        )
        half_hidden, half_first = hidden_grad, first_grad
        hidden_grad, first_grad, bias_sum = exchange(
            "z",
            nz,
            lambda s: part(half_hidden, z ^ s, nz, 0),
            lambda s: part(half_first, z ^ s, nz, 0),
            bias_sum,
        )

        def spread(value, axes, size, me, axis):
            return place([value] + [swap(value, axes, size, s) for s in range(1, size)], me, axis)

        hidden_out = hidden_grad.astype(BF16)
        first_out = first_grad.astype(BF16)
        hidden_out = spread(hidden_out, "z", nz, z, 0)
        first_out = spread(first_out, "z", nz, z, 0)
        hidden_out = spread(hidden_out, "x", nx, x, 0)
        first_out = spread(first_out, "x", nx, x, 0)
        first_out = spread(first_out, "y", ny, y, 1)
        hidden_out = spread(hidden_out, "c", nc, c, 0)
        first_out = spread(first_out, "c", nc, c, 0)
        return (
            first_out.astype(F32),
            bias_sum[ny:].reshape(-1),
            hidden_out.astype(F32),
            bias_sum[y],
            decoder_grad,
        )

    return on_device


def solution(mesh):
    dp, mp = mesh.shape["dp"], mesh.shape["mp"]
    nc = 2 if dp % 2 == 0 else 1
    nx = 2 if dp % (2 * nc) == 0 else 1
    nz = dp // (nc * nx)
    fine = Mesh(mesh.devices.reshape(nz, nx, nc, mp), ("z", "x", "c", "y"))
    dps = ("z", "x", "c")
    every = dps + ("y",)
    placed = (
        P(),
        P(),
        P(None, every),
        P(None, every, None),
        P(),
        P(),
        P(None, "y"),
        P("y"),
        P(every, None),
    )
    pieces = nc * nx * nz

    def step(*args):
        window, weight, part_weight = args[1], args[4], args[6]
        rank, hidden = weight.shape
        packed = nc == nx == mp == 2 and window.shape[0] % nc == 0
        packed = packed and rank % (8 * pieces) == 0 and hidden % (16 * pieces) == 0
        packed = packed and part_weight.shape[1] % 128 == 0
        build = make_fast_step if packed else make_step
        return build(nz, nx, nc, mp)(*args)

    return jax.shard_map(
        step,
        mesh=fine,
        in_specs=placed,
        out_specs=(P(), P(), P(None, "y"), P("y"), P(every, None)),
        check_vma=False,
    )
```

```python
import jax
import jax.numpy as jnp
from jax import lax
from jax.experimental import pallas as pl
from jax.experimental.pallas import tpu as pltpu
from jax.sharding import Mesh, PartitionSpec as P

F32 = jnp.float32
BF16 = jnp.bfloat16


def dot(a, b, contract):
    return lax.dot_general(a, b, (contract, ((), ())), preferred_element_type=F32)


def swap(value, axes, size, step):
    return lax.ppermute(value, axes, [(j, j ^ step) for j in range(size)])


def tree_sum(parts):
    while len(parts) > 1:
        parts = [parts[i] + parts[i + 1] for i in range(0, len(parts), 2)]
    return parts[0]


def place(pieces, me, axis):
    width = pieces[0].shape[axis]
    shape = list(pieces[0].shape)
    shape[axis] *= len(pieces)
    whole = jnp.zeros(shape, pieces[0].dtype)
    for step, piece in enumerate(pieces):
        whole = lax.dynamic_update_slice_in_dim(whole, piece, (me ^ step) * width, axis)
    return whole


def part(value, index, count, axis):
    width = value.shape[axis] // count
    return lax.dynamic_slice_in_dim(value, index * width, width, axis)


VMEM = pl.BlockSpec(memory_space=pltpu.VMEM)
SMEM = pl.BlockSpec(memory_space=pltpu.SMEM)
ANY = pl.BlockSpec(memory_space=pltpu.HBM)


COST_UNIT = 1 << 30


def aligned(index, size):
    return pl.ds(pl.multiple_of(index * size, size), size)


def local_call(body, outs, args, specs=None, scratch=(), limit=24 << 20, cost=1.0):
    return pallas_call(body, outs, args, specs, scratch, limit, cost)


def pallas_call(body, outs, args, specs, scratch, limit, cost):
    return pl.pallas_call(
        body,
        out_shape=[jax.ShapeDtypeStruct(shape, kind) for shape, kind in outs],
        in_specs=[VMEM] * len(args) if specs is None else specs,
        out_specs=[VMEM] * len(outs),
        scratch_shapes=list(scratch),
        compiler_params=pltpu.CompilerParams(vmem_limit_bytes=limit),
        cost_estimate=pl.CostEstimate(
            flops=int(cost * COST_UNIT), bytes_accessed=1 << 20, transcendentals=0
        ),
    )(*args)


def make_fast_step(nz, nx, nc, ny):
    nxy = nx * ny

    def on_device(
        inputs_store,
        window,
        targets_store,
        jac_store,
        first_weight,
        first_bias,
        hidden_weight,
        hidden_bias,
        decoder_weight,
    ):
        rank, hidden = first_weight.shape
        kw = hidden_weight.shape[1]
        outs, depth = decoder_weight.shape[0], inputs_store.shape[0]
        count = window.shape[0] // nc
        total = (count + 1) * rank
        hrow_c, frow_c = hidden // nc, rank // nc
        hrow_x = hrow_c // nx
        hrow_z, frow_z = hrow_x // nz, frow_c // nz
        brow = 16

        def swaps(values, axes, size):
            moved = [values[0]]
            for step in range(1, size):
                moved.append(swap(values[step], axes, size, step))
            return moved

        sent = part(hidden_weight, lax.axis_index("c"), nc, 0)
        got = swap(sent, "y", ny, 1)
        bias_got = swap(hidden_bias, "y", ny, 1)
        decoder_got = swap(decoder_weight, "c", nc, 1)

        def gather(
            window_ref, jac_ref, target_ref, input_ref, weight_ref, bias_ref,
            own_ref, away_ref, act_ref, turned_ref, sems,
        ):
            me = lax.axis_index("c")
            copies = []
            for u, ref in enumerate((away_ref, own_ref)):
                for i in range(count):
                    row = window_ref[(me ^ u ^ 1) * count + i]
                    copies.append(pltpu.make_async_copy(jac_ref.at[row], ref.at[i], sems.at[u, i]))
            for copy in copies:
                copy.start()
            line = lax.broadcasted_iota(jnp.int32, (rank, depth), 0)
            place_of = lax.broadcasted_iota(jnp.int32, (rank, depth), 1)

            def pick(member, table):
                index = jnp.full((rank, depth), -1, jnp.int32)
                for i in range(count):
                    index = jnp.where(line == i, window_ref[member * count + i], index)
                chosen = jnp.where(index == place_of, 1.0, 0.0).astype(BF16)
                return jnp.dot(chosen, table, preferred_element_type=F32)

            inputs = pick(me, input_ref[...])
            turned_ref[...] = inputs.T
            first_pre = jnp.dot(
                inputs.astype(BF16), weight_ref[...], preferred_element_type=F32
            )[:count]
            act_ref[...] = jnp.tanh(first_pre + bias_ref[...].astype(F32).reshape(1, hidden))
            own_ref[count] = pick(me, target_ref[...]).T.astype(BF16)
            away_ref[count] = pick(me ^ 1, target_ref[...]).T.astype(BF16)
            for copy in copies:
                copy.wait()

        jac_shape = ((count + 1,) + jac_store.shape[1:], BF16)
        jac_own, jac_away, first_act, turned = local_call(
            gather,
            [jac_shape, jac_shape, ((count, hidden), F32), ((rank, rank), F32)],
            (window, jac_store, targets_store, inputs_store, first_weight, first_bias),
            cost=4,
            specs=[SMEM, ANY, VMEM, VMEM, VMEM, VMEM],
            scratch=[pltpu.SemaphoreType.DMA((nc, count))],
            limit=60 << 20,
        )
        jac_got = swap(jac_away, "c", nc, 1)

        def warm(act_ref, weight_ref, half_ref, tan_ref, side_ref, lin_ref):
            act = act_ref[...]
            slope = 1.0 - act * act
            weight = weight_ref[...].astype(F32)
            pad = jnp.zeros((rank - count, hidden), F32)
            for s in range(count):
                rows = slice(s * rank, (s + 1) * rank)
                tan_ref[rows] = (slope[s : s + 1] * weight).astype(BF16)
            padded = jnp.concatenate([act, pad])
            tan_ref[count * rank :] = padded.astype(BF16)
            lin_ref[...] = jnp.dot(tan_ref[...], half_ref[...], preferred_element_type=F32)
            slope_side = jnp.concatenate([slope, pad]).T
            weight_side = weight.T
            for s in range(count):
                columns = slice(s * rank, (s + 1) * rank)
                side_ref[:, columns] = (slope_side[:, s : s + 1] * weight_side).astype(BF16)
            side_ref[:, count * rank :] = padded.T.astype(BF16)

        first_tan, first_side, lin_own = local_call(
            warm,
            [((total, hidden), BF16), ((hidden, total), BF16), ((total, kw), F32)],
            (first_act, first_weight, hidden_weight),
            cost=2,
            limit=30 << 20,
        )
        got, bias_got, decoder_got, jac_got, first_tan = lax.optimization_barrier(
            (got, bias_got, decoder_got, jac_got, first_tan)
        )
        got_core = swap(got, "c", nc, 1)

        def main(
            tan1_ref, side_ref, lin_ref, got_ref, core_ref, bias_ref, bias_got_ref,
            dec_ref, dec_got_ref, jac_ref, jac_got_ref,
            half_ref, tan_ref, miss_ref, round_ref, sum_ref, out_ref,
            lin_got_ref, wide_ref, net_ref, back_ref,
        ):
            me, my = lax.axis_index("c"), lax.axis_index("y")
            half_ref[aligned(me, hrow_c)] = got_ref[...]
            half_ref[aligned(me ^ 1, hrow_c)] = core_ref[...]
            for b in range(ny):
                columns = slice(b * kw, (b + 1) * kw)
                wide_ref[:outs, columns] = dec_ref[:, aligned(my ^ b, kw)]
                wide_ref[outs:, columns] = dec_got_ref[:, aligned(my ^ b, kw)]
            lin_got_ref[...] = jnp.dot(tan1_ref[...], half_ref[...], preferred_element_type=F32)
            pad = jnp.zeros((rank - count, kw), F32)
            last = slice(count * rank, total)
            lins, acts, slopes = (lin_ref, lin_got_ref), [], []
            for b, (lin, bias) in enumerate(zip(lins, (bias_ref, bias_got_ref))):
                columns = slice(b * kw, (b + 1) * kw)
                pre = lin[count * rank : count * rank + count]
                act = jnp.tanh(pre + bias[...].astype(F32).reshape(1, kw))
                slope = 1.0 - act * act
                acts.append(act)
                slopes.append(slope)
                tan_ref[last, columns] = jnp.concatenate([act, pad]).astype(BF16)
                for s in range(count):
                    rows = slice(s * rank, (s + 1) * rank)
                    tan_ref[rows, columns] = (slope[s : s + 1] * lin[rows]).astype(BF16)
            net_ref[...] = dot(wide_ref[...], tan_ref[...], ((1,), (1,)))
            for s in range(count + 1):
                columns = slice(s * rank, (s + 1) * rank)
                for part_rows, jac in ((slice(0, outs), jac_ref), (slice(outs, None), jac_got_ref)):
                    miss = net_ref[part_rows, columns] - jac[s].astype(F32)
                    miss_ref[part_rows, columns] = miss.astype(BF16)
            back_ref[...] = dot(miss_ref[...], wide_ref[...], ((0,), (0,)))
            for b, lin in enumerate(lins):
                columns = slice(b * kw, (b + 1) * kw)
                act, slope = acts[b], slopes[b]
                sums = []
                for s in range(count):
                    rows = slice(s * rank, (s + 1) * rank)
                    back = back_ref[rows, columns]
                    sums.append(jnp.sum(back * lin[rows], axis=0, keepdims=True))
                    round_ref[rows, columns] = (back * slope[s : s + 1]).astype(BF16)
                act_back = back_ref[count * rank : count * rank + count, columns]
                sums = jnp.concatenate(sums)
                pre_back = act_back * slope - 2.0 * act * slope * sums
                round_ref[last, columns] = jnp.concatenate([pre_back, pad]).astype(BF16)
                sum_ref[:, columns] = jnp.sum(pre_back, axis=0, keepdims=True)
            out_ref[...] = jnp.dot(
                side_ref[aligned(me ^ 1, hrow_c)], round_ref[...], preferred_element_type=F32
            ).astype(BF16)

        half_got, hidden_tan, miss, lin_round, hidden_sum, g_away = local_call(
            main,
            [
                ((hidden, kw), BF16),
                ((total, hidden), BF16),
                ((nc * outs, total), BF16),
                ((total, hidden), BF16),
                ((1, hidden), F32),
                ((hrow_c, hidden), BF16),
            ],
            (
                first_tan, first_side, lin_own, got, got_core, hidden_bias, bias_got,
                decoder_weight, decoder_got, jac_own, jac_got,
            ),
            cost=6.5,
            scratch=[
                pltpu.VMEM((total, kw), F32),
                pltpu.VMEM((nc * outs, hidden), BF16),
                pltpu.VMEM((nc * outs, total), F32),
                pltpu.VMEM((total, hidden), F32),
            ],
            limit=40 << 20,
        )
        g_got = swap(g_away, "c", nc, 1)

        def own_rows(side_ref, round_ref, out_ref):
            me = lax.axis_index("c")
            out_ref[...] = jnp.dot(
                side_ref[aligned(me, hrow_c)], round_ref[...], preferred_element_type=F32
            )

        (g_own,) = local_call(
            own_rows, [((hrow_c, hidden), F32)], (first_side, lin_round), cost=1.5, limit=16 << 20
        )

        def merge_core(g_ref, got_ref, *out_refs):
            mx = lax.axis_index("x")
            for s, out_ref in enumerate(out_refs):
                a, b = s // ny, s % ny
                rows, columns = aligned(mx ^ a, hrow_x), slice(b * kw, (b + 1) * kw)
                value = g_ref[rows, columns] + got_ref[rows, columns].astype(F32)
                out_ref[...] = value.astype(BF16)

        plane = local_call(merge_core, [((hrow_x, kw), BF16)] * nxy, (g_own, g_got))
        (lin_round, miss, hidden_tan), _ = lax.optimization_barrier(
            ((lin_round, miss, hidden_tan), plane[0])
        )
        plane = swaps(plane, ("x", "y"), nxy)

        def lower(
            round_ref, half_ref, got_ref, act_ref, weight_ref, turned_ref, sum_ref,
            own_ref, away_ref, bias_ref, low_ref, first_ref,
        ):
            me, my = lax.axis_index("c"), lax.axis_index("y")
            low_ref[...] = dot(round_ref[:, :kw], half_ref[...], ((1,), (1,)))
            low_ref[...] += dot(round_ref[:, kw:], got_ref[...], ((1,), (1,)))
            act = act_ref[...]
            slope = 1.0 - act * act
            weight = weight_ref[...].astype(F32)
            sums = []
            for s in range(count):
                low = low_ref[s * rank : (s + 1) * rank]
                sums.append(jnp.sum(low * weight, axis=0, keepdims=True))
            act_lower = low_ref[count * rank : count * rank + count]
            pre_lower = act_lower * slope - 2.0 * act * slope * jnp.concatenate(sums)
            turned = turned_ref[...]
            value = jnp.zeros((rank, hidden), F32)
            for s in range(count):
                low = low_ref[s * rank : (s + 1) * rank]
                value = value + low * slope[s : s + 1]
                value = value + turned[:, s : s + 1] * pre_lower[s : s + 1]
            first_ref[...] = value
            own_ref[...] = first_ref[aligned(me, frow_c)]
            away = first_ref[aligned(me ^ 1, frow_c)].astype(BF16)
            for b in range(ny):
                away_ref[b * frow_c : (b + 1) * frow_c] = away[:, b * kw : (b + 1) * kw]
            sums = sum_ref[...]
            halves = [sums[:, :kw], sums[:, kw:]]
            first_sum = jnp.sum(pre_lower, axis=0, keepdims=True)
            bias = jnp.concatenate(
                [
                    jnp.where(my == 0, halves[0], halves[1]),
                    jnp.where(my == 0, halves[1], halves[0]),
                    first_sum[:, :kw],
                    first_sum[:, kw:],
                    jnp.zeros((brow - 2 * ny, kw), F32),
                ]
            ).astype(BF16)
            away_ref[ny * frow_c :] = bias
            bias_ref[...] = bias

        f_own, f_away, b_own = local_call(
            lower,
            [
                ((frow_c, hidden), F32),
                ((ny * frow_c + brow, kw), BF16),
                ((brow, kw), BF16),
            ],
            (lin_round, hidden_weight, half_got, first_act, first_weight, turned, hidden_sum),
            cost=3,
            scratch=[pltpu.VMEM((total, hidden), F32), pltpu.VMEM((rank, hidden), F32)],
            limit=30 << 20,
        )
        _, f_got = swaps([f_away] * nc, "c", nc)

        def merge_first(f_ref, got_ref, b_ref, *out_refs):
            mz = lax.axis_index("z")
            bias = (b_ref[...].astype(F32) + got_ref[ny * frow_c :].astype(F32)).astype(BF16)
            for s, out_ref in enumerate(out_refs):
                rows = aligned(mz ^ s, frow_z)
                for b in range(ny):
                    there = pl.ds(pl.multiple_of(b * frow_c + (mz ^ s) * frow_z, frow_z), frow_z)
                    value = f_ref[rows, b * kw : (b + 1) * kw] + got_ref[there].astype(F32)
                    out_ref[b * frow_z : (b + 1) * frow_z] = value.astype(BF16)
                out_ref[ny * frow_z :] = bias

        side = local_call(
            merge_first, [((ny * frow_z + brow, kw), BF16)] * nz, (f_own, f_got, b_own)
        )
        side = swaps(side, "z", nz)

        def readout(miss_ref, tan_ref, own_ref, away_ref):
            own_ref[...] = jnp.dot(miss_ref[:outs], tan_ref[...], preferred_element_type=F32)
            away_ref[...] = jnp.dot(miss_ref[outs:], tan_ref[...], preferred_element_type=F32)

        d_own, d_away = local_call(
            readout, [((outs, hidden), F32)] * 2, (miss, hidden_tan), cost=1, limit=16 << 20
        )
        *plane, d_away = lax.optimization_barrier((*plane, d_away))
        d_got = swap(d_away, "c", nc, 1)

        def join(own_ref, got_ref, out_ref):
            my = lax.axis_index("y")
            for b in range(ny):
                columns = slice(b * kw, (b + 1) * kw)
                out_ref[:, aligned(my ^ b, kw)] = own_ref[:, columns] + got_ref[:, columns]

        (decoder_grad,) = local_call(
            join, [((outs, hidden), F32)], (d_own, d_got), cost=1, limit=8 << 20
        )

        def merge_plane(*refs):
            in_refs, out_refs, total_ref = refs[:nxy], refs[nxy:-1], refs[-1]
            mz = lax.axis_index("z")
            total_ref[...] = tree_sum([ref[...].astype(F32) for ref in in_refs])
            for s, out_ref in enumerate(out_refs):
                out_ref[...] = total_ref[aligned(mz ^ s, hrow_z)].astype(BF16)

        line = local_call(
            merge_plane,
            [((hrow_z, kw), BF16)] * nz,
            tuple(plane),
            scratch=[pltpu.VMEM((hrow_x, kw), F32)],
        )
        line = swaps(line, "z", nz)

        def add_rounded(*refs):
            total_sum = tree_sum([ref[...].astype(F32) for ref in refs[:-1]])
            refs[-1][...] = total_sum.astype(BF16)

        (side_sum,) = local_call(add_rounded, [((ny * frow_z + brow, kw), BF16)], tuple(side))
        side = swaps([side_sum] * nxy, ("x", "y"), nxy)
        *line, decoder_grad = lax.optimization_barrier((*line, decoder_grad))
        (piece,) = local_call(add_rounded, [((hrow_z, kw), BF16)], tuple(line))
        pieces = swaps([piece] * nz, "z", nz)

        def finish_side(*refs):
            in_refs, (out_ref, hidden_ref, first_ref) = refs[:nxy], refs[nxy:]
            my = lax.axis_index("y")
            total_sum = tree_sum([ref[...].astype(F32) for ref in in_refs])
            out_ref[...] = total_sum[: ny * frow_z].astype(BF16)
            bias = total_sum[ny * frow_z :]
            hidden_ref[...] = jnp.where(my == 0, bias[0:1], bias[1:2]).reshape(kw)
            for b in range(ny):
                row = bias[ny + b : ny + b + 1]
                first_ref[b * kw : (b + 1) * kw] = row.reshape(kw)

        side_piece, hidden_bias_out, first_bias_out = local_call(
            finish_side, [((ny * frow_z, kw), BF16), ((kw,), F32), ((hidden,), F32)], tuple(side)
        )
        side_pieces = swaps([side_piece] * nz, "z", nz)

        def stack(*refs):
            mz = lax.axis_index("z")
            for s, ref in enumerate(refs[:nz]):
                refs[nz][mz ^ s] = ref[...]

        (both,) = local_call(stack, [((nz, hrow_z, kw), BF16)], tuple(pieces))
        (first,) = local_call(stack, [((nz, ny * frow_z, kw), BF16)], tuple(side_pieces))
        _, across = swaps([both] * nx, "x", nx)
        _, both_core = swaps([both] * nc, "c", nc)
        _, first_core = swaps([first] * nc, "c", nc)
        across, both_core, first_core = lax.optimization_barrier((across, both_core, first_core))
        across_core = swap(across, "c", nc, 1)

        def spread_out(*refs):
            in_refs, side_refs = refs[: nc * nx], refs[nc * nx : nc * nx + nc]
            hidden_ref, first_ref = refs[-2:]
            mx, mc = lax.axis_index("x"), lax.axis_index("c")
            for s, ref in enumerate(in_refs):
                base = (mc ^ (s // nx)) * nx + (mx ^ (s % nx))
                for i in range(nz):
                    hidden_ref[aligned(base * nz + i, hrow_z)] = ref[i].astype(F32)
            for u, ref in enumerate(side_refs):
                for i in range(nz):
                    rows = aligned((mc ^ u) * nz + i, frow_z)
                    value = ref[i].astype(F32)
                    for b in range(ny):
                        first_ref[rows, b * kw : (b + 1) * kw] = value[b * frow_z : (b + 1) * frow_z]

        hidden_out, first_out = local_call(
            spread_out,
            [((hidden, kw), F32), ((rank, hidden), F32)],
            (both, across, both_core, across_core, first, first_core),
            cost=2,
        )
        return (first_out, first_bias_out, hidden_out, hidden_bias_out, decoder_grad)

    return on_device


def make_step(nz, nx, nc, ny):
    nxy = nx * ny

    def on_device(
        inputs_store,
        window,
        targets_store,
        jac_store,
        first_weight,
        first_bias,
        hidden_weight,
        hidden_bias,
        decoder_weight,
    ):
        z, x, c, y = (lax.axis_index(name) for name in ("z", "x", "c", "y"))
        rank, hidden = first_weight.shape
        kw = hidden_weight.shape[1]
        pieces = [hidden_weight]
        biases = [hidden_bias]
        mine = part(hidden_weight, c, nc, 0)
        for t in range(1, ny):
            got = swap(mine, "y", ny, t)
            rest = [got] + [swap(got, "c", nc, u) for u in range(1, nc)]
            pieces.append(place(rest, c, 0))
            biases.append(swap(hidden_bias, "y", ny, t))
        wide_hidden = jnp.concatenate(pieces, axis=1)
        wide_bias = jnp.concatenate(biases)
        jac_parts, target_parts, decoder_parts = [], [], []
        for u in range(nc):
            rows = part(window, c ^ u, nc, 0)
            jac, target = jac_store[rows], targets_store[rows]
            decoder = decoder_weight
            if u:
                jac, target, decoder = (swap(v, "c", nc, u) for v in (jac, target, decoder))
            jac_parts.append(jac)
            target_parts.append(target)
            decoder_parts.append(decoder)
        jac = jnp.concatenate(jac_parts, axis=1)
        target = jnp.concatenate(target_parts, axis=1)
        decoder = jnp.concatenate(decoder_parts, axis=0)
        decoder = jnp.concatenate([part(decoder, y ^ t, ny, 1) for t in range(ny)], axis=1)
        inputs = inputs_store[part(window, c, nc, 0)]
        count = inputs.shape[0]
        weight_one = first_weight.astype(F32)
        first_act = jnp.tanh(dot(inputs, first_weight, ((1,), (0,))) + first_bias.astype(F32))
        first_slope = 1.0 - first_act * first_act
        first_tan = (first_slope[:, None, :] * weight_one[None]).astype(BF16)
        first_tan = first_tan.reshape(count * rank, hidden)
        first_round = first_act.astype(BF16)
        hidden_lin = dot(first_tan, wide_hidden, ((1,), (0,))).reshape(count, rank, -1)
        hidden_act = jnp.tanh(
            dot(first_round, wide_hidden, ((1,), (0,))) + wide_bias.astype(F32)
        )
        hidden_slope = 1.0 - hidden_act * hidden_act
        hidden_tan = (hidden_slope[:, None, :] * hidden_lin).astype(BF16)
        hidden_round = hidden_act.astype(BF16)
        output_miss = dot(hidden_round, decoder, ((1,), (1,))) - target.astype(F32)
        output_miss = output_miss.astype(BF16)
        jac_net = dot(decoder, hidden_tan, ((1,), (2,)))
        jac_miss = (jac_net - jac.transpose(1, 0, 2).astype(F32)).astype(BF16)
        jac_miss = jac_miss.reshape(-1, count * rank)
        grad = dot(output_miss, hidden_round, ((0,), (0,))) + dot(
            jac_miss, hidden_tan.reshape(count * rank, -1), ((1,), (0,))
        )
        blocks = jnp.split(grad, nc, axis=0)
        own = [blocks[0]] + [swap(blocks[u], "c", nc, u) for u in range(1, nc)]
        grad = tree_sum(own)
        decoder_grad = place(jnp.split(grad, ny, axis=1), y, 1)

        act_back = dot(output_miss, decoder, ((1,), (0,)))
        tan_back = dot(jac_miss, decoder, ((0,), (0,))).reshape(count, rank, -1)
        pre_back = act_back * hidden_slope - 2.0 * hidden_act * hidden_slope * jnp.sum(
            tan_back * hidden_lin, axis=1
        )
        lin_round = (tan_back * hidden_slope[:, None, :]).astype(BF16)
        lin_round = lin_round.reshape(count * rank, -1)
        pre_round = pre_back.astype(BF16)
        hidden_grad = dot(first_round, pre_round, ((0,), (0,))) + dot(
            first_tan, lin_round, ((0,), (0,))
        )
        tan_lower = dot(lin_round, wide_hidden, ((1,), (1,))).reshape(count, rank, hidden)
        act_lower = dot(pre_round, wide_hidden, ((1,), (1,)))
        pre_lower = act_lower * first_slope - 2.0 * first_act * first_slope * jnp.sum(
            tan_lower * weight_one[None], axis=1
        )
        first_grad = jnp.einsum(
            "sr,sh->rh", inputs.astype(F32), pre_lower, precision=lax.Precision.HIGHEST
        ) + jnp.sum(tan_lower * first_slope[:, None, :], axis=0)
        hidden_bsum = jnp.sum(pre_back, axis=0).reshape(ny, kw)
        hidden_bsum = place([hidden_bsum[t : t + 1] for t in range(ny)], y, 0)
        first_bsum = jnp.sum(pre_lower, axis=0).reshape(ny, kw)
        bias_sum = jnp.concatenate([hidden_bsum, first_bsum])

        def exchange(axes, size, hidden_of, first_of, bias):
            totals = []
            for s in range(size):
                sent = (hidden_of(s), first_of(s), bias)
                sent = [v.astype(BF16) for v in sent]
                if s:
                    sent = [swap(v, axes, size, s) for v in sent]
                totals.append([v.astype(F32) for v in sent])
            return [tree_sum(list(group)) for group in zip(*totals)]

        hidden_grad, first_grad, bias_sum = exchange(
            "c",
            nc,
            lambda s: part(hidden_grad, c ^ s, nc, 0),
            lambda s: part(first_grad, c ^ s, nc, 0),
            bias_sum,
        )
        whole_hidden, whole_first = hidden_grad, first_grad
        hidden_grad, first_grad, bias_sum = exchange(
            ("x", "y"),
            nxy,
            lambda s: part(whole_hidden, x ^ (s // ny), nx, 0)[
                :, (s % ny) * kw : (s % ny + 1) * kw
            ],
            lambda s: part(part(whole_first, x ^ (s // ny), nx, 0), y ^ (s % ny), ny, 1),
            bias_sum,
        )
        half_hidden, half_first = hidden_grad, first_grad
        hidden_grad, first_grad, bias_sum = exchange(
            "z",
            nz,
            lambda s: part(half_hidden, z ^ s, nz, 0),
            lambda s: part(half_first, z ^ s, nz, 0),
            bias_sum,
        )

        def spread(value, axes, size, me, axis):
            return place([value] + [swap(value, axes, size, s) for s in range(1, size)], me, axis)

        hidden_out = hidden_grad.astype(BF16)
        first_out = first_grad.astype(BF16)
        hidden_out = spread(hidden_out, "z", nz, z, 0)
        first_out = spread(first_out, "z", nz, z, 0)
        hidden_out = spread(hidden_out, "x", nx, x, 0)
        first_out = spread(first_out, "x", nx, x, 0)
        first_out = spread(first_out, "y", ny, y, 1)
        hidden_out = spread(hidden_out, "c", nc, c, 0)
        first_out = spread(first_out, "c", nc, c, 0)
        return (
            first_out.astype(F32),
            bias_sum[ny:].reshape(-1),
            hidden_out.astype(F32),
            bias_sum[y],
            decoder_grad,
        )

    return on_device


def solution(mesh):
    dp, mp = mesh.shape["dp"], mesh.shape["mp"]
    nc = 2 if dp % 2 == 0 else 1
    nx = 2 if dp % (2 * nc) == 0 else 1
    nz = dp // (nc * nx)
    fine = Mesh(mesh.devices.reshape(nz, nx, nc, mp), ("z", "x", "c", "y"))
    dps = ("z", "x", "c")
    every = dps + ("y",)
    placed = (
        P(),
        P(),
        P(None, every),
        P(None, every, None),
        P(),
        P(),
        P(None, "y"),
        P("y"),
        P(every, None),
    )
    pieces = nc * nx * nz

    def step(*args):
        window, weight, part_weight = args[1], args[4], args[6]
        rank, hidden = weight.shape
        packed = nc == nx == mp == 2 and window.shape[0] % nc == 0
        packed = packed and rank % (8 * pieces) == 0 and hidden % (16 * pieces) == 0
        packed = packed and part_weight.shape[1] % 128 == 0
        build = make_fast_step if packed else make_step
        return build(nz, nx, nc, mp)(*args)

    return jax.shard_map(
        step,
        mesh=fine,
        in_specs=placed,
        out_specs=(P(), P(), P(None, "y"), P("y"), P(every, None)),
        check_vma=False,
    )
```

```python
import jax
import jax.numpy as jnp
from jax import lax
from jax.experimental import pallas as pl
from jax.experimental.pallas import tpu as pltpu
from jax.sharding import Mesh, PartitionSpec as P

F32 = jnp.float32
BF16 = jnp.bfloat16


def dot(a, b, contract):
    return lax.dot_general(a, b, (contract, ((), ())), preferred_element_type=F32)


def swap(value, axes, size, step):
    return lax.ppermute(value, axes, [(j, j ^ step) for j in range(size)])


def tree_sum(parts):
    while len(parts) > 1:
        parts = [parts[i] + parts[i + 1] for i in range(0, len(parts), 2)]
    return parts[0]


def place(pieces, me, axis):
    width = pieces[0].shape[axis]
    shape = list(pieces[0].shape)
    shape[axis] *= len(pieces)
    whole = jnp.zeros(shape, pieces[0].dtype)
    for step, piece in enumerate(pieces):
        whole = lax.dynamic_update_slice_in_dim(whole, piece, (me ^ step) * width, axis)
    return whole


def part(value, index, count, axis):
    width = value.shape[axis] // count
    return lax.dynamic_slice_in_dim(value, index * width, width, axis)


VMEM = pl.BlockSpec(memory_space=pltpu.VMEM)
SMEM = pl.BlockSpec(memory_space=pltpu.SMEM)
ANY = pl.BlockSpec(memory_space=pltpu.HBM)


COST_UNIT = 1 << 30


def aligned(index, size):
    return pl.ds(pl.multiple_of(index * size, size), size)


def local_call(body, outs, args, **options):
    return kernel_call(body, outs, args, **options)


def kernel_call(
    body, outs, args, specs=None, out_specs=None, scratch=(), aliases=None, limit=24 << 20, cost=1.0
):
    return pl.pallas_call(
        body,
        out_shape=[jax.ShapeDtypeStruct(shape, kind) for shape, kind in outs],
        in_specs=[VMEM] * len(args) if specs is None else specs,
        out_specs=[VMEM] * len(outs) if out_specs is None else out_specs,
        input_output_aliases=aliases or {},
        scratch_shapes=list(scratch),
        compiler_params=pltpu.CompilerParams(vmem_limit_bytes=limit),
        cost_estimate=pl.CostEstimate(
            flops=int(cost * COST_UNIT), bytes_accessed=1 << 20, transcendentals=0
        ),
    )(*args)


def make_fast_step(nz, nx, nc, ny):
    nxy = nx * ny

    def on_device(
        inputs_store,
        window,
        targets_store,
        jac_store,
        first_weight,
        first_bias,
        hidden_weight,
        hidden_bias,
        decoder_weight,
    ):
        rank, hidden = first_weight.shape
        kw = hidden_weight.shape[1]
        outs, depth = decoder_weight.shape[0], inputs_store.shape[0]
        count = window.shape[0] // nc
        total = (count + 1) * rank
        hrow_c, frow_c = hidden // nc, rank // nc
        hrow_x = hrow_c // nx
        hrow_z, frow_z = hrow_x // nz, frow_c // nz
        brow = 16

        def swaps(values, axes, size):
            moved = [values[0]]
            for step in range(1, size):
                moved.append(swap(values[step], axes, size, step))
            return moved

        shared = hrow_c // 2
        near_rows = shared // nx
        c, x = lax.axis_index("c"), lax.axis_index("x")
        near = lax.dynamic_slice_in_dim(hidden_weight, c * hrow_c + x * near_rows, near_rows)
        rest = lax.dynamic_slice_in_dim(
            hidden_weight, c * hrow_c + shared - brow, hrow_c - shared + brow
        )
        line = lax.broadcasted_iota(jnp.int32, rest.shape, 0)
        rest = jnp.where(line < brow, hidden_bias[None, :], rest)
        _, near_got = swaps([near] * ny, "y", ny)
        _, rest_got = swaps([rest] * ny, "y", ny)
        _, decoder_got = swaps([decoder_weight] * nc, "c", nc)
        _, far_got = swaps([near_got] * nx, "x", nx)

        def gather(
            window_ref, jac_ref, target_ref, input_ref, weight_ref, bias_ref,
            own_ref, away_ref, act_ref, turned_ref, sems,
        ):
            me = lax.axis_index("c")
            copies = []
            for u, ref in enumerate((away_ref, own_ref)):
                for i in range(count):
                    row = window_ref[(me ^ u ^ 1) * count + i]
                    copies.append(pltpu.make_async_copy(jac_ref.at[row], ref.at[i], sems.at[u, i]))
            for copy in copies:
                copy.start()
            padded_rows = -(-count // 16) * 16
            line = lax.broadcasted_iota(jnp.int32, (padded_rows, depth), 0)
            place_of = lax.broadcasted_iota(jnp.int32, (padded_rows, depth), 1)
            pad = jnp.zeros((rank - padded_rows, rank), F32)

            def pick(member, table):
                index = jnp.full((padded_rows, depth), -1, jnp.int32)
                for i in range(count):
                    index = jnp.where(line == i, window_ref[member * count + i], index)
                chosen = jnp.where(index == place_of, 1.0, 0.0).astype(BF16)
                return jnp.dot(chosen, table, preferred_element_type=F32)

            inputs = pick(me, input_ref[...])
            turned_ref[...] = jnp.concatenate([inputs, pad]).T
            first_pre = jnp.dot(
                inputs.astype(BF16), weight_ref[...], preferred_element_type=F32
            )[:count]
            act_ref[...] = jnp.tanh(first_pre + bias_ref[...].astype(F32).reshape(1, hidden))
            for member, ref in ((me, own_ref), (me ^ 1, away_ref)):
                target = jnp.concatenate([pick(member, target_ref[...]), pad])
                ref[count] = target.T.astype(BF16)
            for copy in copies:
                copy.wait()

        jac_shape = ((count + 1,) + jac_store.shape[1:], BF16)
        jac_own, jac_away, first_act, turned = local_call(
            gather,
            [jac_shape, jac_shape, ((count, hidden), F32), ((rank, rank), F32)],
            (window, jac_store, targets_store, inputs_store, first_weight, first_bias),
            cost=4,
            specs=[SMEM, ANY, VMEM, VMEM, VMEM, VMEM],
            scratch=[pltpu.SemaphoreType.DMA((nc, count))],
            limit=60 << 20,
        )
        _, jac_got = swaps([jac_away] * nc, "c", nc)

        def warm(act_ref, weight_ref, half_ref, tan_ref, side_ref, lin_ref):
            act = act_ref[...]
            slope = 1.0 - act * act
            weight = weight_ref[...].astype(F32)
            pad = jnp.zeros((rank - count, hidden), F32)
            for s in range(count):
                rows = slice(s * rank, (s + 1) * rank)
                tan_ref[rows] = (slope[s : s + 1] * weight).astype(BF16)
            padded = jnp.concatenate([act, pad])
            tan_ref[count * rank :] = padded.astype(BF16)
            lin_ref[...] = jnp.dot(tan_ref[...], half_ref[...], preferred_element_type=F32)
            slope_side = jnp.concatenate([slope, pad]).T
            weight_side = weight.T
            for s in range(count):
                columns = slice(s * rank, (s + 1) * rank)
                side_ref[:, columns] = (slope_side[:, s : s + 1] * weight_side).astype(BF16)
            side_ref[:, count * rank :] = padded.T.astype(BF16)

        first_tan, first_side, lin_own = local_call(
            warm,
            [((total, hidden), BF16), ((hidden, total), BF16), ((total, kw), F32)],
            (first_act, first_weight, hidden_weight),
            cost=2,
            limit=30 << 20,
        )

        def ready(
            lin_ref, bias_ref, dec_ref, dec_got_ref, jac_ref, jac_got_ref,
            wide_ref, tan_ref, net_ref,
        ):
            my = lax.axis_index("y")
            for b in range(ny):
                columns = slice(b * kw, (b + 1) * kw)
                wide_ref[:outs, columns] = dec_ref[:, aligned(my ^ b, kw)]
                wide_ref[outs:, columns] = dec_got_ref[:, aligned(my ^ b, kw)]
            hidden_tangents(lin_ref, *hidden_slopes(lin_ref, hidden_row(bias_ref)), tan_ref)
            net_ref[...] = dot(wide_ref[:, :kw], tan_ref[...], ((1,), (1,)))
            for s in range(count + 1):
                columns = slice(s * rank, (s + 1) * rank)
                net_ref[:outs, columns] -= jac_ref[s].astype(F32)
                net_ref[outs:, columns] -= jac_got_ref[s].astype(F32)

        def hidden_row(bias_ref):
            return bias_ref[...].astype(F32).reshape(1, kw)

        def hidden_slopes(lin_ref, bias):
            act = jnp.tanh(lin_ref[count * rank : count * rank + count] + bias)
            return act, 1.0 - act * act

        def hidden_tangents(lin_ref, act, slope, tan_ref):
            pad = jnp.zeros((rank - count, kw), F32)
            for s in range(count):
                rows = slice(s * rank, (s + 1) * rank)
                tan_ref[rows] = (slope[s : s + 1] * lin_ref[rows]).astype(BF16)
            tan_ref[count * rank :] = jnp.concatenate([act, pad]).astype(BF16)

        wide, tan_own, net_own = local_call(
            ready,
            [((nc * outs, hidden), BF16), ((total, kw), BF16), ((nc * outs, total), F32)],
            (lin_own, hidden_bias, decoder_weight, decoder_got, jac_own, jac_got),
            cost=1.5,
            limit=16 << 20,
        )
        near_got, rest_got, far_got, tan_own = lax.optimization_barrier(
            (near_got, rest_got, far_got, tan_own)
        )
        fetched = (near_got, far_got, rest_got)
        fetched += tuple(swap(value, "c", nc, 1) for value in fetched)

        def main(
            tan1_ref, side_ref, lin_ref, near_ref, far_ref, rest_ref, near2_ref, far2_ref, rest2_ref,
            bias_ref, wide_ref, net_own_ref,
            half_ref, tan_ref, miss_ref, round_ref, sum_ref, out_ref,
            lin_got_ref, back_ref,
        ):
            me, mx = lax.axis_index("c"), lax.axis_index("x")
            for u, refs in enumerate(((near_ref, far_ref, rest_ref), (near2_ref, far2_ref, rest2_ref))):
                base = (me ^ u) * hrow_c
                for a in range(nx):
                    start = pl.multiple_of(base + (mx ^ a) * near_rows, near_rows)
                    half_ref[pl.ds(start, near_rows)] = refs[a][...]
                start = pl.multiple_of(base + shared, shared)
                half_ref[pl.ds(start, hrow_c - shared)] = refs[2][brow:]
            lin_got_ref[...] = jnp.dot(tan1_ref[...], half_ref[...], preferred_element_type=F32)
            bias_got = rest_ref[:brow].astype(F32)[:1]
            own, other = hidden_slopes(lin_ref, hidden_row(bias_ref)), hidden_slopes(lin_got_ref, bias_got)
            hidden_tangents(lin_got_ref, *other, tan_ref)
            net = net_own_ref[...] + dot(wide_ref[:, kw:], tan_ref[...], ((1,), (1,)))
            miss_ref[...] = net.astype(BF16)
            back_ref[...] = dot(miss_ref[...], wide_ref[...], ((0,), (0,)))
            pad = jnp.zeros((rank - count, kw), F32)
            for b, (lin, (act, slope)) in enumerate(((lin_ref, own), (lin_got_ref, other))):
                columns = slice(b * kw, (b + 1) * kw)
                sums = []
                for s in range(count):
                    rows = slice(s * rank, (s + 1) * rank)
                    back = back_ref[rows, columns]
                    sums.append(jnp.sum(back * lin[rows], axis=0, keepdims=True))
                    round_ref[rows, columns] = (back * slope[s : s + 1]).astype(BF16)
                act_back = back_ref[count * rank : count * rank + count, columns]
                pre_back = act_back * slope - 2.0 * act * slope * jnp.concatenate(sums)
                round_ref[count * rank :, columns] = jnp.concatenate([pre_back, pad]).astype(BF16)
                sum_ref[:, columns] = jnp.sum(pre_back, axis=0, keepdims=True)
            out_ref[...] = jnp.dot(
                side_ref[aligned(me ^ 1, hrow_c)], round_ref[:, kw:], preferred_element_type=F32
            ).astype(BF16)

        half_got, tan_got, miss, lin_round, hidden_sum, g_away = local_call(
            main,
            [
                ((hidden, kw), BF16),
                ((total, kw), BF16),
                ((nc * outs, total), BF16),
                ((total, hidden), BF16),
                ((1, hidden), F32),
                ((hrow_c, kw), BF16),
            ],
            (first_tan, first_side, lin_own, *fetched, hidden_bias, wide, net_own),
            cost=5,
            scratch=[pltpu.VMEM((total, kw), F32), pltpu.VMEM((total, hidden), F32)],
            limit=36 << 20,
        )
        _, g_got = swaps([g_away] * nc, "c", nc)

        def between(side_ref, round_ref, own_ref, away_ref):
            me = lax.axis_index("c")
            own_ref[...] = jnp.dot(
                side_ref[aligned(me, hrow_c)], round_ref[:, kw:], preferred_element_type=F32
            )
            away_ref[...] = jnp.dot(
                side_ref[aligned(me ^ 1, hrow_c)], round_ref[:, :kw], preferred_element_type=F32
            ).astype(BF16)

        g_own, g_away = local_call(
            between,
            [((hrow_c, kw), F32), ((hrow_c, kw), BF16)],
            (first_side, lin_round),
            cost=1.5,
            limit=16 << 20,
        )
        _, g_got_last = swaps([g_away] * nc, "c", nc)

        def merge_core(g_ref, got_ref, *out_refs):
            mx = lax.axis_index("x")
            for a, out_ref in enumerate(out_refs):
                rows = aligned(mx ^ a, hrow_x)
                out_ref[...] = (g_ref[rows] + got_ref[rows].astype(F32)).astype(BF16)

        rows_shape = ((hrow_x, kw), BF16)
        plane1, plane3 = local_call(merge_core, [rows_shape] * nx, (g_own, g_got))

        def finish_core(side_ref, round_ref, got_ref, *refs):
            me, g_ref = lax.axis_index("c"), refs[-1]
            g_ref[...] = jnp.dot(
                side_ref[aligned(me, hrow_c)], round_ref[:, :kw], preferred_element_type=F32
            )
            merge_core(g_ref, got_ref, *refs[:-1])

        plane0, plane2 = local_call(
            finish_core,
            [rows_shape] * nx,
            (first_side, lin_round, g_got_last),
            scratch=[pltpu.VMEM((hrow_c, kw), F32)],
            limit=16 << 20,
        )
        plane = [plane0, plane1, plane2, plane3]
        (lin_round, miss, tan_got), _ = lax.optimization_barrier(
            ((lin_round, miss, tan_got), plane[0])
        )
        plane = swaps(plane, ("x", "y"), nxy)

        def lower(
            round_ref, half_ref, got_ref, act_ref, weight_ref, turned_ref, sum_ref,
            own_ref, away_ref, bias_ref, low_ref, first_ref,
        ):
            me, my = lax.axis_index("c"), lax.axis_index("y")
            low_ref[...] = dot(round_ref[:, :kw], half_ref[...], ((1,), (1,)))
            low_ref[...] += dot(round_ref[:, kw:], got_ref[...], ((1,), (1,)))
            act = act_ref[...]
            slope = 1.0 - act * act
            weight = weight_ref[...].astype(F32)
            sums = []
            for s in range(count):
                low = low_ref[s * rank : (s + 1) * rank]
                sums.append(jnp.sum(low * weight, axis=0, keepdims=True))
            act_lower = low_ref[count * rank : count * rank + count]
            pre_lower = act_lower * slope - 2.0 * act * slope * jnp.concatenate(sums)
            turned = turned_ref[...]
            value = jnp.zeros((rank, hidden), F32)
            for s in range(count):
                low = low_ref[s * rank : (s + 1) * rank]
                value = value + low * slope[s : s + 1]
                value = value + turned[:, s : s + 1] * pre_lower[s : s + 1]
            first_ref[...] = value
            own_ref[...] = first_ref[aligned(me, frow_c)]
            away = first_ref[aligned(me ^ 1, frow_c)].astype(BF16)
            for b in range(ny):
                away_ref[b * frow_c : (b + 1) * frow_c] = away[:, b * kw : (b + 1) * kw]
            sums = sum_ref[...]
            halves = [sums[:, :kw], sums[:, kw:]]
            first_sum = jnp.sum(pre_lower, axis=0, keepdims=True)
            bias = jnp.concatenate(
                [
                    jnp.where(my == 0, halves[0], halves[1]),
                    jnp.where(my == 0, halves[1], halves[0]),
                    first_sum[:, :kw],
                    first_sum[:, kw:],
                    jnp.zeros((brow - 2 * ny, kw), F32),
                ]
            ).astype(BF16)
            away_ref[ny * frow_c :] = bias
            bias_ref[...] = bias

        f_own, f_away, b_own = local_call(
            lower,
            [
                ((frow_c, hidden), F32),
                ((ny * frow_c + brow, kw), BF16),
                ((brow, kw), BF16),
            ],
            (lin_round, hidden_weight, half_got, first_act, first_weight, turned, hidden_sum),
            cost=3,
            scratch=[pltpu.VMEM((total, hidden), F32), pltpu.VMEM((rank, hidden), F32)],
            limit=30 << 20,
        )
        _, f_got = swaps([f_away] * nc, "c", nc)

        def merge_first(f_ref, got_ref, b_ref, *out_refs):
            mz = lax.axis_index("z")
            bias = (b_ref[...].astype(F32) + got_ref[ny * frow_c :].astype(F32)).astype(BF16)
            for s, out_ref in enumerate(out_refs):
                rows = aligned(mz ^ s, frow_z)
                for b in range(ny):
                    there = pl.ds(pl.multiple_of(b * frow_c + (mz ^ s) * frow_z, frow_z), frow_z)
                    value = f_ref[rows, b * kw : (b + 1) * kw] + got_ref[there].astype(F32)
                    out_ref[b * frow_z : (b + 1) * frow_z] = value.astype(BF16)
                out_ref[ny * frow_z :] = bias

        side = local_call(
            merge_first, [((ny * frow_z + brow, kw), BF16)] * nz, (f_own, f_got, b_own)
        )
        side = swaps(side, "z", nz)

        def readout(miss_ref, tan_ref, tan_got_ref, own_ref, away_ref):
            for ref, rows in ((own_ref, slice(0, outs)), (away_ref, slice(outs, None))):
                for b, tan in enumerate((tan_ref, tan_got_ref)):
                    ref[:, b * kw : (b + 1) * kw] = jnp.dot(
                        miss_ref[rows], tan[...], preferred_element_type=F32
                    )

        d_own, d_away = local_call(
            readout, [((outs, hidden), F32)] * 2, (miss, tan_own, tan_got), cost=1, limit=16 << 20
        )
        *plane, d_away = lax.optimization_barrier((*plane, d_away))
        d_got = swap(d_away, "c", nc, 1)

        def join(own_ref, got_ref, out_ref):
            my = lax.axis_index("y")
            for b in range(ny):
                columns = slice(b * kw, (b + 1) * kw)
                out_ref[:, aligned(my ^ b, kw)] = own_ref[:, columns] + got_ref[:, columns]

        (decoder_grad,) = local_call(
            join, [((outs, hidden), F32)], (d_own, d_got), cost=1, limit=8 << 20
        )

        def merge_plane(*refs):
            in_refs, out_refs, total_ref = refs[:nxy], refs[nxy:-1], refs[-1]
            mz = lax.axis_index("z")
            total_ref[...] = tree_sum([ref[...].astype(F32) for ref in in_refs])
            for s, out_ref in enumerate(out_refs):
                out_ref[...] = total_ref[aligned(mz ^ s, hrow_z)].astype(BF16)

        line = local_call(
            merge_plane,
            [((hrow_z, kw), BF16)] * nz,
            tuple(plane),
            scratch=[pltpu.VMEM((hrow_x, kw), F32)],
        )
        line = swaps(line, "z", nz)

        def add_rounded(*refs):
            total_sum = tree_sum([ref[...].astype(F32) for ref in refs[:-1]])
            refs[-1][...] = total_sum.astype(BF16)

        (side_sum,) = local_call(add_rounded, [((ny * frow_z + brow, kw), BF16)], tuple(side))
        side = swaps([side_sum] * nxy, ("x", "y"), nxy)
        *line, decoder_grad = lax.optimization_barrier((*line, decoder_grad))
        (piece,) = local_call(add_rounded, [((hrow_z, kw), BF16)], tuple(line))
        pieces = swaps([piece] * nz, "z", nz)

        def finish_side(*refs):
            in_refs, (out_ref, hidden_ref, first_ref) = refs[:nxy], refs[nxy:]
            my = lax.axis_index("y")
            total_sum = tree_sum([ref[...].astype(F32) for ref in in_refs])
            out_ref[...] = total_sum[: ny * frow_z].astype(BF16)
            bias = total_sum[ny * frow_z :]
            hidden_ref[...] = jnp.where(my == 0, bias[0:1], bias[1:2]).reshape(kw)
            for b in range(ny):
                row = bias[ny + b : ny + b + 1]
                first_ref[b * kw : (b + 1) * kw] = row.reshape(kw)

        side_piece, hidden_bias_out, first_bias_out = local_call(
            finish_side, [((ny * frow_z, kw), BF16), ((kw,), F32), ((hidden,), F32)], tuple(side)
        )
        side_pieces = swaps([side_piece] * nz, "z", nz)

        def stack(*refs):
            mz = lax.axis_index("z")
            for s, ref in enumerate(refs[:nz]):
                refs[nz][mz ^ s] = ref[...]

        (both,) = local_call(stack, [((nz, hrow_z, kw), BF16)], tuple(pieces))
        (first,) = local_call(stack, [((nz, ny * frow_z, kw), BF16)], tuple(side_pieces))
        _, across = swaps([both] * nx, "x", nx)
        _, both_core = swaps([both] * nc, "c", nc)
        _, first_core = swaps([first] * nc, "c", nc)
        across_core = swap(across, "c", nc, 1)

        def put(refs, base, size, out_ref, stage_ref, sem_ref, slot):
            copies = []
            for i in range(nz):
                stage_ref[slot * nz + i] = refs[i].astype(F32)
                copies.append(
                    pltpu.make_async_copy(
                        stage_ref.at[slot * nz + i],
                        out_ref.at[aligned(base * nz + i, size)],
                        sem_ref.at[slot * nz + i],
                    )
                )
                copies[-1].start()
            return copies

        def spread_early(both_ref, core_ref, out_ref, stage_ref, sem_ref):
            mx, mc = lax.axis_index("x"), lax.axis_index("c")
            copies = put(both_ref, mc * nx + mx, hrow_z, out_ref, stage_ref, sem_ref, 0)
            copies += put(core_ref, (mc ^ 1) * nx + mx, hrow_z, out_ref, stage_ref, sem_ref, 1)
            for copy in copies:
                copy.wait()

        stage = [pltpu.VMEM((nc * nz, hrow_z, kw), F32), pltpu.SemaphoreType.DMA((nc * nz,))]

        def spread_first(own_ref, core_ref, first_ref):
            mc = lax.axis_index("c")
            for u, ref in enumerate((own_ref, core_ref)):
                for i in range(nz):
                    rows = aligned((mc ^ u) * nz + i, frow_z)
                    value = ref[i].astype(F32)
                    for b in range(ny):
                        first_ref[rows, b * kw : (b + 1) * kw] = value[b * frow_z : (b + 1) * frow_z]

        def spread_late(held_ref, across_ref, core_ref, out_ref, stage_ref, sem_ref):
            mx, mc = lax.axis_index("x"), lax.axis_index("c")
            copies = put(across_ref, mc * nx + (mx ^ 1), hrow_z, out_ref, stage_ref, sem_ref, 0)
            copies += put(core_ref, (mc ^ 1) * nx + (mx ^ 1), hrow_z, out_ref, stage_ref, sem_ref, 1)
            for copy in copies:
                copy.wait()

        (hidden_out,) = local_call(
            spread_early,
            [((hidden, kw), F32)],
            (both, both_core),
            out_specs=[ANY],
            scratch=stage,
            limit=8 << 20,
        )
        (first_out,) = local_call(
            spread_first, [((rank, hidden), F32)], (first, first_core), limit=4 << 20
        )
        (hidden_out,) = local_call(
            spread_late,
            [((hidden, kw), F32)],
            (hidden_out, across, across_core),
            specs=[ANY, VMEM, VMEM],
            out_specs=[ANY],
            scratch=stage,
            aliases={0: 0},
            limit=8 << 20,
        )
        return (first_out, first_bias_out, hidden_out, hidden_bias_out, decoder_grad)

    return on_device


def make_step(nz, nx, nc, ny):
    nxy = nx * ny

    def on_device(
        inputs_store,
        window,
        targets_store,
        jac_store,
        first_weight,
        first_bias,
        hidden_weight,
        hidden_bias,
        decoder_weight,
    ):
        z, x, c, y = (lax.axis_index(name) for name in ("z", "x", "c", "y"))
        rank, hidden = first_weight.shape
        kw = hidden_weight.shape[1]
        pieces = [hidden_weight]
        biases = [hidden_bias]
        mine = part(hidden_weight, c, nc, 0)
        for t in range(1, ny):
            got = swap(mine, "y", ny, t)
            rest = [got] + [swap(got, "c", nc, u) for u in range(1, nc)]
            pieces.append(place(rest, c, 0))
            biases.append(swap(hidden_bias, "y", ny, t))
        wide_hidden = jnp.concatenate(pieces, axis=1)
        wide_bias = jnp.concatenate(biases)
        jac_parts, target_parts, decoder_parts = [], [], []
        for u in range(nc):
            rows = part(window, c ^ u, nc, 0)
            jac, target = jac_store[rows], targets_store[rows]
            decoder = decoder_weight
            if u:
                jac, target, decoder = (swap(v, "c", nc, u) for v in (jac, target, decoder))
            jac_parts.append(jac)
            target_parts.append(target)
            decoder_parts.append(decoder)
        jac = jnp.concatenate(jac_parts, axis=1)
        target = jnp.concatenate(target_parts, axis=1)
        decoder = jnp.concatenate(decoder_parts, axis=0)
        decoder = jnp.concatenate([part(decoder, y ^ t, ny, 1) for t in range(ny)], axis=1)
        inputs = inputs_store[part(window, c, nc, 0)]
        count = inputs.shape[0]
        weight_one = first_weight.astype(F32)
        first_act = jnp.tanh(dot(inputs, first_weight, ((1,), (0,))) + first_bias.astype(F32))
        first_slope = 1.0 - first_act * first_act
        first_tan = (first_slope[:, None, :] * weight_one[None]).astype(BF16)
        first_tan = first_tan.reshape(count * rank, hidden)
        first_round = first_act.astype(BF16)
        hidden_lin = dot(first_tan, wide_hidden, ((1,), (0,))).reshape(count, rank, -1)
        hidden_act = jnp.tanh(
            dot(first_round, wide_hidden, ((1,), (0,))) + wide_bias.astype(F32)
        )
        hidden_slope = 1.0 - hidden_act * hidden_act
        hidden_tan = (hidden_slope[:, None, :] * hidden_lin).astype(BF16)
        hidden_round = hidden_act.astype(BF16)
        output_miss = dot(hidden_round, decoder, ((1,), (1,))) - target.astype(F32)
        output_miss = output_miss.astype(BF16)
        jac_net = dot(decoder, hidden_tan, ((1,), (2,)))
        jac_miss = (jac_net - jac.transpose(1, 0, 2).astype(F32)).astype(BF16)
        jac_miss = jac_miss.reshape(-1, count * rank)
        grad = dot(output_miss, hidden_round, ((0,), (0,))) + dot(
            jac_miss, hidden_tan.reshape(count * rank, -1), ((1,), (0,))
        )
        blocks = jnp.split(grad, nc, axis=0)
        own = [blocks[0]] + [swap(blocks[u], "c", nc, u) for u in range(1, nc)]
        grad = tree_sum(own)
        decoder_grad = place(jnp.split(grad, ny, axis=1), y, 1)

        act_back = dot(output_miss, decoder, ((1,), (0,)))
        tan_back = dot(jac_miss, decoder, ((0,), (0,))).reshape(count, rank, -1)
        pre_back = act_back * hidden_slope - 2.0 * hidden_act * hidden_slope * jnp.sum(
            tan_back * hidden_lin, axis=1
        )
        lin_round = (tan_back * hidden_slope[:, None, :]).astype(BF16)
        lin_round = lin_round.reshape(count * rank, -1)
        pre_round = pre_back.astype(BF16)
        hidden_grad = dot(first_round, pre_round, ((0,), (0,))) + dot(
            first_tan, lin_round, ((0,), (0,))
        )
        tan_lower = dot(lin_round, wide_hidden, ((1,), (1,))).reshape(count, rank, hidden)
        act_lower = dot(pre_round, wide_hidden, ((1,), (1,)))
        pre_lower = act_lower * first_slope - 2.0 * first_act * first_slope * jnp.sum(
            tan_lower * weight_one[None], axis=1
        )
        first_grad = jnp.einsum(
            "sr,sh->rh", inputs.astype(F32), pre_lower, precision=lax.Precision.HIGHEST
        ) + jnp.sum(tan_lower * first_slope[:, None, :], axis=0)
        hidden_bsum = jnp.sum(pre_back, axis=0).reshape(ny, kw)
        hidden_bsum = place([hidden_bsum[t : t + 1] for t in range(ny)], y, 0)
        first_bsum = jnp.sum(pre_lower, axis=0).reshape(ny, kw)
        bias_sum = jnp.concatenate([hidden_bsum, first_bsum])

        def exchange(axes, size, hidden_of, first_of, bias):
            totals = []
            for s in range(size):
                sent = (hidden_of(s), first_of(s), bias)
                sent = [v.astype(BF16) for v in sent]
                if s:
                    sent = [swap(v, axes, size, s) for v in sent]
                totals.append([v.astype(F32) for v in sent])
            return [tree_sum(list(group)) for group in zip(*totals)]

        hidden_grad, first_grad, bias_sum = exchange(
            "c",
            nc,
            lambda s: part(hidden_grad, c ^ s, nc, 0),
            lambda s: part(first_grad, c ^ s, nc, 0),
            bias_sum,
        )
        whole_hidden, whole_first = hidden_grad, first_grad
        hidden_grad, first_grad, bias_sum = exchange(
            ("x", "y"),
            nxy,
            lambda s: part(whole_hidden, x ^ (s // ny), nx, 0)[
                :, (s % ny) * kw : (s % ny + 1) * kw
            ],
            lambda s: part(part(whole_first, x ^ (s // ny), nx, 0), y ^ (s % ny), ny, 1),
            bias_sum,
        )
        half_hidden, half_first = hidden_grad, first_grad
        hidden_grad, first_grad, bias_sum = exchange(
            "z",
            nz,
            lambda s: part(half_hidden, z ^ s, nz, 0),
            lambda s: part(half_first, z ^ s, nz, 0),
            bias_sum,
        )

        def spread(value, axes, size, me, axis):
            return place([value] + [swap(value, axes, size, s) for s in range(1, size)], me, axis)

        hidden_out = hidden_grad.astype(BF16)
        first_out = first_grad.astype(BF16)
        hidden_out = spread(hidden_out, "z", nz, z, 0)
        first_out = spread(first_out, "z", nz, z, 0)
        hidden_out = spread(hidden_out, "x", nx, x, 0)
        first_out = spread(first_out, "x", nx, x, 0)
        first_out = spread(first_out, "y", ny, y, 1)
        hidden_out = spread(hidden_out, "c", nc, c, 0)
        first_out = spread(first_out, "c", nc, c, 0)
        return (
            first_out.astype(F32),
            bias_sum[ny:].reshape(-1),
            hidden_out.astype(F32),
            bias_sum[y],
            decoder_grad,
        )

    return on_device


def solution(mesh):
    dp, mp = mesh.shape["dp"], mesh.shape["mp"]
    nc = 2 if dp % 2 == 0 else 1
    nx = 2 if dp % (2 * nc) == 0 else 1
    nz = dp // (nc * nx)
    fine = Mesh(mesh.devices.reshape(nz, nx, nc, mp), ("z", "x", "c", "y"))
    dps = ("z", "x", "c")
    every = dps + ("y",)
    placed = (
        P(),
        P(),
        P(None, every),
        P(None, every, None),
        P(),
        P(),
        P(None, "y"),
        P("y"),
        P(every, None),
    )
    pieces = nc * nx * nz

    def step(*args):
        window, weight, part_weight = args[1], args[4], args[6]
        rank, hidden = weight.shape
        packed = nc == nx == mp == 2 and window.shape[0] % nc == 0
        packed = packed and rank % (8 * pieces) == 0 and hidden % (16 * pieces) == 0
        packed = packed and part_weight.shape[1] % 128 == 0
        build = make_fast_step if packed else make_step
        return build(nz, nx, nc, mp)(*args)

    return jax.shard_map(
        step,
        mesh=fine,
        in_specs=placed,
        out_specs=(P(), P(), P(None, "y"), P("y"), P(every, None)),
        check_vma=False,
    )
```

```python
import jax
import jax.numpy as jnp
from jax import lax
from jax.experimental import pallas as pl
from jax.experimental.pallas import tpu as pltpu
from jax.sharding import Mesh, PartitionSpec as P

F32 = jnp.float32
BF16 = jnp.bfloat16


def dot(a, b, contract):
    return lax.dot_general(a, b, (contract, ((), ())), preferred_element_type=F32)


def swap(value, axes, size, step):
    return lax.ppermute(value, axes, [(j, j ^ step) for j in range(size)])


def tree_sum(parts):
    while len(parts) > 1:
        parts = [parts[i] + parts[i + 1] for i in range(0, len(parts), 2)]
    return parts[0]


def place(pieces, me, axis):
    width = pieces[0].shape[axis]
    shape = list(pieces[0].shape)
    shape[axis] *= len(pieces)
    whole = jnp.zeros(shape, pieces[0].dtype)
    for step, piece in enumerate(pieces):
        whole = lax.dynamic_update_slice_in_dim(whole, piece, (me ^ step) * width, axis)
    return whole


def part(value, index, count, axis):
    width = value.shape[axis] // count
    return lax.dynamic_slice_in_dim(value, index * width, width, axis)


VMEM = pl.BlockSpec(memory_space=pltpu.VMEM)
SMEM = pl.BlockSpec(memory_space=pltpu.SMEM)
ANY = pl.BlockSpec(memory_space=pltpu.HBM)


COST_UNIT = 1 << 30


def aligned(index, size):
    return pl.ds(pl.multiple_of(index * size, size), size)


def local_call(body, outs, args, **options):
    return kernel_call(body, outs, args, **options)


def kernel_call(
    body, outs, args, specs=None, out_specs=None, scratch=(), aliases=None, limit=24 << 20, cost=1.0
):
    return pl.pallas_call(
        body,
        out_shape=[jax.ShapeDtypeStruct(shape, kind) for shape, kind in outs],
        in_specs=[VMEM] * len(args) if specs is None else specs,
        out_specs=[VMEM] * len(outs) if out_specs is None else out_specs,
        input_output_aliases=aliases or {},
        scratch_shapes=list(scratch),
        compiler_params=pltpu.CompilerParams(vmem_limit_bytes=limit),
        cost_estimate=pl.CostEstimate(
            flops=int(cost * COST_UNIT), bytes_accessed=1 << 20, transcendentals=0
        ),
    )(*args)


def make_fast_step(nz, nx, nc, ny):
    nxy = nx * ny

    def on_device(
        inputs_store,
        window,
        targets_store,
        jac_store,
        first_weight,
        first_bias,
        hidden_weight,
        hidden_bias,
        decoder_weight,
    ):
        rank, hidden = first_weight.shape
        kw = hidden_weight.shape[1]
        outs, depth = decoder_weight.shape[0], inputs_store.shape[0]
        count = window.shape[0] // nc
        total = (count + 1) * rank
        hrow_c, frow_c = hidden // nc, rank // nc
        hrow_x = hrow_c // nx
        hrow_z, frow_z = hrow_x // nz, frow_c // nz
        brow, lead = 8, 16

        def swaps(values, axes, size):
            moved = [values[0]]
            for step in range(1, size):
                moved.append(swap(values[step], axes, size, step))
            return moved

        shared = hrow_c // 2
        near_rows = shared // nx
        c, x = lax.axis_index("c"), lax.axis_index("x")
        near = lax.dynamic_slice_in_dim(hidden_weight, c * hrow_c + x * near_rows, near_rows)

        def hand_on(in_ref, out_ref):
            out_ref[...] = in_ref[...]

        (near,) = local_call(hand_on, [((near_rows, kw), BF16)], (near,), cost=20, limit=4 << 20)
        rest = lax.dynamic_slice_in_dim(
            hidden_weight, c * hrow_c + shared - lead, hrow_c - shared + lead
        )
        line = lax.broadcasted_iota(jnp.int32, rest.shape, 0)
        rest = jnp.where(line < lead, hidden_bias[None, :], rest)
        _, near_got = swaps([near] * ny, "y", ny)
        _, rest_got = swaps([rest] * ny, "y", ny)
        _, decoder_got = swaps([decoder_weight] * nc, "c", nc)
        _, far_got = swaps([near_got] * nx, "x", nx)
        _, near_core = swaps([near_got] * nc, "c", nc)

        def gather(
            window_ref, jac_ref, target_ref, input_ref, weight_ref, bias_ref,
            own_ref, away_ref, act_ref, turned_ref, sems,
        ):
            me = lax.axis_index("c")
            copies = []
            for u, ref in enumerate((away_ref, own_ref)):
                for i in range(count):
                    row = window_ref[(me ^ u ^ 1) * count + i]
                    copies.append(pltpu.make_async_copy(jac_ref.at[row], ref.at[i], sems.at[u, i]))
            for copy in copies:
                copy.start()
            padded_rows = -(-count // 16) * 16
            line = lax.broadcasted_iota(jnp.int32, (padded_rows, depth), 0)
            place_of = lax.broadcasted_iota(jnp.int32, (padded_rows, depth), 1)
            pad = jnp.zeros((rank - padded_rows, rank), F32)

            def pick(member, table):
                index = jnp.full((padded_rows, depth), -1, jnp.int32)
                for i in range(count):
                    index = jnp.where(line == i, window_ref[member * count + i], index)
                chosen = jnp.where(index == place_of, 1.0, 0.0).astype(BF16)
                return jnp.dot(chosen, table, preferred_element_type=F32)

            inputs = pick(me, input_ref[...])
            turned_ref[...] = jnp.concatenate([inputs, pad]).T
            first_pre = jnp.dot(
                inputs.astype(BF16), weight_ref[...], preferred_element_type=F32
            )[:count]
            act_ref[...] = jnp.tanh(first_pre + bias_ref[...].astype(F32).reshape(1, hidden))
            for member, ref in ((me, own_ref), (me ^ 1, away_ref)):
                target = jnp.concatenate([pick(member, target_ref[...]), pad])
                ref[count] = target.T.astype(BF16)
            for copy in copies:
                copy.wait()

        jac_shape = ((count + 1,) + jac_store.shape[1:], BF16)
        jac_own, jac_away, first_act, turned = local_call(
            gather,
            [jac_shape, jac_shape, ((count, hidden), F32), ((rank, rank), F32)],
            (window, jac_store, targets_store, inputs_store, first_weight, first_bias),
            cost=4,
            specs=[SMEM, ANY, VMEM, VMEM, VMEM, VMEM],
            scratch=[pltpu.SemaphoreType.DMA((nc, count))],
            limit=50 << 20,
        )
        _, jac_got = swaps([jac_away] * nc, "c", nc)

        def warm(act_ref, weight_ref, half_ref, tan_ref, side_ref, lin_ref):
            act = act_ref[...]
            slope = 1.0 - act * act
            weight = weight_ref[...].astype(F32)
            pad = jnp.zeros((rank - count, hidden), F32)
            for s in range(count):
                rows = slice(s * rank, (s + 1) * rank)
                tan_ref[rows] = (slope[s : s + 1] * weight).astype(BF16)
            padded = jnp.concatenate([act, pad])
            tan_ref[count * rank :] = padded.astype(BF16)
            lin_ref[...] = jnp.dot(tan_ref[...], half_ref[...], preferred_element_type=F32)
            slope_side = jnp.concatenate([slope, pad]).T
            weight_side = weight.T
            for s in range(count):
                columns = slice(s * rank, (s + 1) * rank)
                side_ref[:, columns] = (slope_side[:, s : s + 1] * weight_side).astype(BF16)
            side_ref[:, count * rank :] = padded.T.astype(BF16)

        first_tan, first_side, lin_own = local_call(
            warm,
            [((total, hidden), BF16), ((hidden, total), BF16), ((total, kw), F32)],
            (first_act, first_weight, hidden_weight),
            cost=2,
            limit=30 << 20,
        )

        def ready(
            lin_ref, bias_ref, dec_ref, dec_got_ref, jac_ref, jac_got_ref,
            wide_ref, tan_ref, net_ref,
        ):
            my = lax.axis_index("y")
            for b in range(ny):
                columns = slice(b * kw, (b + 1) * kw)
                wide_ref[:outs, columns] = dec_ref[:, aligned(my ^ b, kw)]
                wide_ref[outs:, columns] = dec_got_ref[:, aligned(my ^ b, kw)]
            hidden_tangents(lin_ref, *hidden_slopes(lin_ref, hidden_row(bias_ref)), tan_ref)
            net_ref[...] = dot(wide_ref[:, :kw], tan_ref[...], ((1,), (1,)))
            for s in range(count + 1):
                columns = slice(s * rank, (s + 1) * rank)
                net_ref[:outs, columns] -= jac_ref[s].astype(F32)
                net_ref[outs:, columns] -= jac_got_ref[s].astype(F32)

        def hidden_row(bias_ref):
            return bias_ref[...].astype(F32).reshape(1, kw)

        def hidden_slopes(lin_ref, bias):
            act = jnp.tanh(lin_ref[count * rank : count * rank + count] + bias)
            return act, 1.0 - act * act

        def hidden_tangents(lin_ref, act, slope, tan_ref):
            pad = jnp.zeros((rank - count, kw), F32)
            for s in range(count):
                rows = slice(s * rank, (s + 1) * rank)
                tan_ref[rows] = (slope[s : s + 1] * lin_ref[rows]).astype(BF16)
            tan_ref[count * rank :] = jnp.concatenate([act, pad]).astype(BF16)

        wide, tan_own, net_own = local_call(
            ready,
            [((nc * outs, hidden), BF16), ((total, kw), BF16), ((nc * outs, total), F32)],
            (lin_own, hidden_bias, decoder_weight, decoder_got, jac_own, jac_got),
            cost=1.5,
            limit=16 << 20,
        )
        rest_got, far_got, tan_own = lax.optimization_barrier((rest_got, far_got, tan_own))
        fetched = (near_got, far_got, rest_got, near_core)
        fetched += tuple(swap(value, "c", nc, 1) for value in (far_got, rest_got))

        def main(
            tan1_ref, side_ref, lin_ref, near_ref, far_ref, rest_ref, near2_ref, far2_ref, rest2_ref,
            bias_ref, wide_ref, net_own_ref,
            half_ref, tan_ref, miss_ref, round_ref, sum_ref, out_ref,
            lin_got_ref, back_ref,
        ):
            me, mx = lax.axis_index("c"), lax.axis_index("x")
            for u, refs in enumerate(((near_ref, far_ref, rest_ref), (near2_ref, far2_ref, rest2_ref))):
                base = (me ^ u) * hrow_c
                for a in range(nx):
                    start = pl.multiple_of(base + (mx ^ a) * near_rows, near_rows)
                    half_ref[pl.ds(start, near_rows)] = refs[a][...]
                start = pl.multiple_of(base + shared, shared)
                half_ref[pl.ds(start, hrow_c - shared)] = refs[2][lead:]
            lin_got_ref[...] = jnp.dot(tan1_ref[...], half_ref[...], preferred_element_type=F32)
            bias_got = rest_ref[:lead].astype(F32)[:1]
            own, other = hidden_slopes(lin_ref, hidden_row(bias_ref)), hidden_slopes(lin_got_ref, bias_got)
            hidden_tangents(lin_got_ref, *other, tan_ref)
            net = net_own_ref[...] + dot(wide_ref[:, kw:], tan_ref[...], ((1,), (1,)))
            miss_ref[...] = net.astype(BF16)
            back_ref[...] = dot(miss_ref[...], wide_ref[...], ((0,), (0,)))
            pad = jnp.zeros((rank - count, kw), F32)
            for b, (lin, (act, slope)) in enumerate(((lin_ref, own), (lin_got_ref, other))):
                columns = slice(b * kw, (b + 1) * kw)
                sums = []
                for s in range(count):
                    rows = slice(s * rank, (s + 1) * rank)
                    back = back_ref[rows, columns]
                    sums.append(jnp.sum(back * lin[rows], axis=0, keepdims=True))
                    round_ref[rows, columns] = (back * slope[s : s + 1]).astype(BF16)
                act_back = back_ref[count * rank : count * rank + count, columns]
                pre_back = act_back * slope - 2.0 * act * slope * jnp.concatenate(sums)
                round_ref[count * rank :, columns] = jnp.concatenate([pre_back, pad]).astype(BF16)
                sum_ref[:, columns] = jnp.sum(pre_back, axis=0, keepdims=True)
            out_ref[...] = jnp.dot(
                side_ref[aligned(me ^ 1, hrow_c)], round_ref[:, kw:], preferred_element_type=F32
            ).astype(BF16)

        half_got, tan_got, miss, lin_round, hidden_sum, g_away = local_call(
            main,
            [
                ((hidden, kw), BF16),
                ((total, kw), BF16),
                ((nc * outs, total), BF16),
                ((total, hidden), BF16),
                ((1, hidden), F32),
                ((hrow_c, kw), BF16),
            ],
            (first_tan, first_side, lin_own, *fetched, hidden_bias, wide, net_own),
            cost=5,
            scratch=[pltpu.VMEM((total, kw), F32), pltpu.VMEM((total, hidden), F32)],
            limit=36 << 20,
        )
        _, g_got = swaps([g_away] * nc, "c", nc)

        def between(side_ref, round_ref, own_ref, away_ref):
            me = lax.axis_index("c")
            own_ref[...] = jnp.dot(
                side_ref[aligned(me, hrow_c)], round_ref[:, kw:], preferred_element_type=F32
            )
            away_ref[...] = jnp.dot(
                side_ref[aligned(me ^ 1, hrow_c)], round_ref[:, :kw], preferred_element_type=F32
            ).astype(BF16)

        g_own, g_away = local_call(
            between,
            [((hrow_c, kw), F32), ((hrow_c, kw), BF16)],
            (first_side, lin_round),
            cost=1.5,
            limit=16 << 20,
        )
        _, g_got_last = swaps([g_away] * nc, "c", nc)

        def merge_core(g_ref, got_ref, *out_refs):
            mx = lax.axis_index("x")
            for a, out_ref in enumerate(out_refs):
                rows = aligned(mx ^ a, hrow_x)
                out_ref[...] = (g_ref[rows] + got_ref[rows].astype(F32)).astype(BF16)

        rows_shape = ((hrow_x, kw), BF16)
        plane1, plane3 = local_call(merge_core, [rows_shape] * nx, (g_own, g_got))

        def finish_core(side_ref, round_ref, got_ref, *refs):
            me, g_ref = lax.axis_index("c"), refs[-1]
            g_ref[...] = jnp.dot(
                side_ref[aligned(me, hrow_c)], round_ref[:, :kw], preferred_element_type=F32
            )
            merge_core(g_ref, got_ref, *refs[:-1])

        plane0, plane2 = local_call(
            finish_core,
            [rows_shape] * nx,
            (first_side, lin_round, g_got_last),
            scratch=[pltpu.VMEM((hrow_c, kw), F32)],
            limit=16 << 20,
        )
        plane = [plane0, plane1, plane2, plane3]
        (lin_round, miss, tan_got), _ = lax.optimization_barrier(
            ((lin_round, miss, tan_got), plane[0])
        )
        plane = swaps(plane, ("x", "y"), nxy)

        def lower(
            round_ref, half_ref, got_ref, act_ref, weight_ref, turned_ref, sum_ref,
            own_ref, away_ref, bias_ref, low_ref, first_ref,
        ):
            me, my = lax.axis_index("c"), lax.axis_index("y")
            low_ref[...] = dot(round_ref[:, :kw], half_ref[...], ((1,), (1,)))
            low_ref[...] += dot(round_ref[:, kw:], got_ref[...], ((1,), (1,)))
            act = act_ref[...]
            slope = 1.0 - act * act
            weight = weight_ref[...].astype(F32)
            sums = []
            for s in range(count):
                low = low_ref[s * rank : (s + 1) * rank]
                sums.append(jnp.sum(low * weight, axis=0, keepdims=True))
            act_lower = low_ref[count * rank : count * rank + count]
            pre_lower = act_lower * slope - 2.0 * act * slope * jnp.concatenate(sums)
            turned = turned_ref[...]
            value = jnp.zeros((rank, hidden), F32)
            for s in range(count):
                low = low_ref[s * rank : (s + 1) * rank]
                value = value + low * slope[s : s + 1]
                value = value + turned[:, s : s + 1] * pre_lower[s : s + 1]
            first_ref[...] = value
            own_ref[...] = first_ref[aligned(me, frow_c)]
            away = first_ref[aligned(me ^ 1, frow_c)].astype(BF16)
            for b in range(ny):
                away_ref[b * frow_c : (b + 1) * frow_c] = away[:, b * kw : (b + 1) * kw]
            sums = sum_ref[...]
            halves = [sums[:, :kw], sums[:, kw:]]
            first_sum = jnp.sum(pre_lower, axis=0, keepdims=True)
            bias = jnp.concatenate(
                [
                    jnp.where(my == 0, halves[0], halves[1]),
                    jnp.where(my == 0, halves[1], halves[0]),
                    first_sum[:, :kw],
                    first_sum[:, kw:],
                    jnp.zeros((brow - 2 * ny, kw), F32),
                ]
            ).astype(BF16)
            away_ref[ny * frow_c :] = bias
            bias_ref[...] = bias

        f_own, f_away, b_own = local_call(
            lower,
            [
                ((frow_c, hidden), F32),
                ((ny * frow_c + brow, kw), BF16),
                ((brow, kw), BF16),
            ],
            (lin_round, hidden_weight, half_got, first_act, first_weight, turned, hidden_sum),
            cost=3,
            scratch=[pltpu.VMEM((total, hidden), F32), pltpu.VMEM((rank, hidden), F32)],
            limit=30 << 20,
        )
        _, f_got = swaps([f_away] * nc, "c", nc)

        def merge_first(f_ref, got_ref, b_ref, *out_refs):
            mz = lax.axis_index("z")
            bias = (b_ref[...].astype(F32) + got_ref[ny * frow_c :].astype(F32)).astype(BF16)
            for s, out_ref in enumerate(out_refs):
                rows = aligned(mz ^ s, frow_z)
                for b in range(ny):
                    there = pl.ds(pl.multiple_of(b * frow_c + (mz ^ s) * frow_z, frow_z), frow_z)
                    value = f_ref[rows, b * kw : (b + 1) * kw] + got_ref[there].astype(F32)
                    out_ref[b * frow_z : (b + 1) * frow_z] = value.astype(BF16)
                out_ref[ny * frow_z :] = bias

        side = local_call(
            merge_first, [((ny * frow_z + brow, kw), BF16)] * nz, (f_own, f_got, b_own)
        )
        side = swaps(side, "z", nz)

        def readout(miss_ref, tan_ref, tan_got_ref, own_ref, away_ref):
            for ref, rows in ((own_ref, slice(0, outs)), (away_ref, slice(outs, None))):
                for b, tan in enumerate((tan_ref, tan_got_ref)):
                    ref[:, b * kw : (b + 1) * kw] = jnp.dot(
                        miss_ref[rows], tan[...], preferred_element_type=F32
                    )

        d_own, d_away = local_call(
            readout, [((outs, hidden), F32)] * 2, (miss, tan_own, tan_got), cost=1, limit=16 << 20
        )
        *plane, d_away = lax.optimization_barrier((*plane, d_away))
        d_got = swap(d_away, "c", nc, 1)

        def join(own_ref, got_ref, out_ref):
            my = lax.axis_index("y")
            for b in range(ny):
                columns = slice(b * kw, (b + 1) * kw)
                out_ref[:, aligned(my ^ b, kw)] = own_ref[:, columns] + got_ref[:, columns]

        (decoder_grad,) = local_call(
            join, [((outs, hidden), F32)], (d_own, d_got), cost=1, limit=8 << 20
        )

        def merge_plane(*refs):
            in_refs, out_refs, total_ref = refs[:nxy], refs[nxy:-1], refs[-1]
            mz = lax.axis_index("z")
            total_ref[...] = tree_sum([ref[...].astype(F32) for ref in in_refs])
            for s, out_ref in enumerate(out_refs):
                out_ref[...] = total_ref[aligned(mz ^ s, hrow_z)].astype(BF16)

        line = local_call(
            merge_plane,
            [((hrow_z, kw), BF16)] * nz,
            tuple(plane),
            scratch=[pltpu.VMEM((hrow_x, kw), F32)],
        )
        line = swaps(line, "z", nz)

        def add_rounded(*refs):
            total_sum = tree_sum([ref[...].astype(F32) for ref in refs[:-1]])
            refs[-1][...] = total_sum.astype(BF16)

        (side_sum,) = local_call(add_rounded, [((ny * frow_z + brow, kw), BF16)], tuple(side))
        side = swaps([side_sum] * nxy, ("x", "y"), nxy)
        *line, decoder_grad = lax.optimization_barrier((*line, decoder_grad))
        (piece,) = local_call(add_rounded, [((hrow_z, kw), BF16)], tuple(line))
        pieces = swaps([piece] * nz, "z", nz)

        def finish_side(*refs):
            in_refs, (out_ref, hidden_ref, first_ref) = refs[:nxy], refs[nxy:]
            my = lax.axis_index("y")
            total_sum = tree_sum([ref[...].astype(F32) for ref in in_refs])
            out_ref[...] = total_sum[: ny * frow_z].astype(BF16)
            bias = total_sum[ny * frow_z :]
            hidden_ref[...] = jnp.where(my == 0, bias[0:1], bias[1:2]).reshape(kw)
            for b in range(ny):
                row = bias[ny + b : ny + b + 1]
                first_ref[b * kw : (b + 1) * kw] = row.reshape(kw)

        side_piece, hidden_bias_out, first_bias_out = local_call(
            finish_side, [((ny * frow_z, kw), BF16), ((kw,), F32), ((hidden,), F32)], tuple(side)
        )
        side_pieces = swaps([side_piece] * nz, "z", nz)

        def stack(*refs):
            mz = lax.axis_index("z")
            for s, ref in enumerate(refs[:nz]):
                refs[nz][mz ^ s] = ref[...]

        (both,) = local_call(stack, [((nz, hrow_z, kw), BF16)], tuple(pieces))
        (first,) = local_call(stack, [((nz, ny * frow_z, kw), BF16)], tuple(side_pieces))
        _, across = swaps([both] * nx, "x", nx)
        _, both_core = swaps([both] * nc, "c", nc)
        _, first_core = swaps([first] * nc, "c", nc)
        _, across_core = swaps([across] * nc, "c", nc)

        def put(refs, base, size, out_ref, stage_ref, sem_ref, slot):
            copies = []
            for i in range(nz):
                stage_ref[slot * nz + i] = refs[i].astype(F32)
                copies.append(
                    pltpu.make_async_copy(
                        stage_ref.at[slot * nz + i],
                        out_ref.at[aligned(base * nz + i, size)],
                        sem_ref.at[slot * nz + i],
                    )
                )
                copies[-1].start()
            return copies

        def spread_early(both_ref, core_ref, out_ref, stage_ref, sem_ref):
            mx, mc = lax.axis_index("x"), lax.axis_index("c")
            copies = put(both_ref, mc * nx + mx, hrow_z, out_ref, stage_ref, sem_ref, 0)
            copies += put(core_ref, (mc ^ 1) * nx + mx, hrow_z, out_ref, stage_ref, sem_ref, 1)
            for copy in copies:
                copy.wait()

        stage = [pltpu.VMEM((nc * nz, hrow_z, kw), F32), pltpu.SemaphoreType.DMA((nc * nz,))]

        def spread_first(own_ref, core_ref, first_ref):
            mc = lax.axis_index("c")
            for u, ref in enumerate((own_ref, core_ref)):
                for i in range(nz):
                    rows = aligned((mc ^ u) * nz + i, frow_z)
                    value = ref[i].astype(F32)
                    for b in range(ny):
                        first_ref[rows, b * kw : (b + 1) * kw] = value[b * frow_z : (b + 1) * frow_z]

        def spread_late(held_ref, across_ref, core_ref, out_ref, stage_ref, sem_ref):
            mx, mc = lax.axis_index("x"), lax.axis_index("c")
            copies = put(across_ref, mc * nx + (mx ^ 1), hrow_z, out_ref, stage_ref, sem_ref, 0)
            copies += put(core_ref, (mc ^ 1) * nx + (mx ^ 1), hrow_z, out_ref, stage_ref, sem_ref, 1)
            for copy in copies:
                copy.wait()

        (hidden_out,) = local_call(
            spread_early,
            [((hidden, kw), F32)],
            (both, both_core),
            out_specs=[ANY],
            scratch=stage,
            limit=8 << 20,
        )
        (first_out,) = local_call(
            spread_first, [((rank, hidden), F32)], (first, first_core), limit=4 << 20
        )
        (hidden_out,) = local_call(
            spread_late,
            [((hidden, kw), F32)],
            (hidden_out, across, across_core),
            specs=[ANY, VMEM, VMEM],
            out_specs=[ANY],
            scratch=stage,
            aliases={0: 0},
            limit=8 << 20,
        )
        return (first_out, first_bias_out, hidden_out, hidden_bias_out, decoder_grad)

    return on_device


def make_step(nz, nx, nc, ny):
    nxy = nx * ny

    def on_device(
        inputs_store,
        window,
        targets_store,
        jac_store,
        first_weight,
        first_bias,
        hidden_weight,
        hidden_bias,
        decoder_weight,
    ):
        z, x, c, y = (lax.axis_index(name) for name in ("z", "x", "c", "y"))
        rank, hidden = first_weight.shape
        kw = hidden_weight.shape[1]
        pieces = [hidden_weight]
        biases = [hidden_bias]
        mine = part(hidden_weight, c, nc, 0)
        for t in range(1, ny):
            got = swap(mine, "y", ny, t)
            rest = [got] + [swap(got, "c", nc, u) for u in range(1, nc)]
            pieces.append(place(rest, c, 0))
            biases.append(swap(hidden_bias, "y", ny, t))
        wide_hidden = jnp.concatenate(pieces, axis=1)
        wide_bias = jnp.concatenate(biases)
        jac_parts, target_parts, decoder_parts = [], [], []
        for u in range(nc):
            rows = part(window, c ^ u, nc, 0)
            jac, target = jac_store[rows], targets_store[rows]
            decoder = decoder_weight
            if u:
                jac, target, decoder = (swap(v, "c", nc, u) for v in (jac, target, decoder))
            jac_parts.append(jac)
            target_parts.append(target)
            decoder_parts.append(decoder)
        jac = jnp.concatenate(jac_parts, axis=1)
        target = jnp.concatenate(target_parts, axis=1)
        decoder = jnp.concatenate(decoder_parts, axis=0)
        decoder = jnp.concatenate([part(decoder, y ^ t, ny, 1) for t in range(ny)], axis=1)
        inputs = inputs_store[part(window, c, nc, 0)]
        count = inputs.shape[0]
        weight_one = first_weight.astype(F32)
        first_act = jnp.tanh(dot(inputs, first_weight, ((1,), (0,))) + first_bias.astype(F32))
        first_slope = 1.0 - first_act * first_act
        first_tan = (first_slope[:, None, :] * weight_one[None]).astype(BF16)
        first_tan = first_tan.reshape(count * rank, hidden)
        first_round = first_act.astype(BF16)
        hidden_lin = dot(first_tan, wide_hidden, ((1,), (0,))).reshape(count, rank, -1)
        hidden_act = jnp.tanh(
            dot(first_round, wide_hidden, ((1,), (0,))) + wide_bias.astype(F32)
        )
        hidden_slope = 1.0 - hidden_act * hidden_act
        hidden_tan = (hidden_slope[:, None, :] * hidden_lin).astype(BF16)
        hidden_round = hidden_act.astype(BF16)
        output_miss = dot(hidden_round, decoder, ((1,), (1,))) - target.astype(F32)
        output_miss = output_miss.astype(BF16)
        jac_net = dot(decoder, hidden_tan, ((1,), (2,)))
        jac_miss = (jac_net - jac.transpose(1, 0, 2).astype(F32)).astype(BF16)
        jac_miss = jac_miss.reshape(-1, count * rank)
        grad = dot(output_miss, hidden_round, ((0,), (0,))) + dot(
            jac_miss, hidden_tan.reshape(count * rank, -1), ((1,), (0,))
        )
        blocks = jnp.split(grad, nc, axis=0)
        own = [blocks[0]] + [swap(blocks[u], "c", nc, u) for u in range(1, nc)]
        grad = tree_sum(own)
        decoder_grad = place(jnp.split(grad, ny, axis=1), y, 1)

        act_back = dot(output_miss, decoder, ((1,), (0,)))
        tan_back = dot(jac_miss, decoder, ((0,), (0,))).reshape(count, rank, -1)
        pre_back = act_back * hidden_slope - 2.0 * hidden_act * hidden_slope * jnp.sum(
            tan_back * hidden_lin, axis=1
        )
        lin_round = (tan_back * hidden_slope[:, None, :]).astype(BF16)
        lin_round = lin_round.reshape(count * rank, -1)
        pre_round = pre_back.astype(BF16)
        hidden_grad = dot(first_round, pre_round, ((0,), (0,))) + dot(
            first_tan, lin_round, ((0,), (0,))
        )
        tan_lower = dot(lin_round, wide_hidden, ((1,), (1,))).reshape(count, rank, hidden)
        act_lower = dot(pre_round, wide_hidden, ((1,), (1,)))
        pre_lower = act_lower * first_slope - 2.0 * first_act * first_slope * jnp.sum(
            tan_lower * weight_one[None], axis=1
        )
        first_grad = jnp.einsum(
            "sr,sh->rh", inputs.astype(F32), pre_lower, precision=lax.Precision.HIGHEST
        ) + jnp.sum(tan_lower * first_slope[:, None, :], axis=0)
        hidden_bsum = jnp.sum(pre_back, axis=0).reshape(ny, kw)
        hidden_bsum = place([hidden_bsum[t : t + 1] for t in range(ny)], y, 0)
        first_bsum = jnp.sum(pre_lower, axis=0).reshape(ny, kw)
        bias_sum = jnp.concatenate([hidden_bsum, first_bsum])

        def exchange(axes, size, hidden_of, first_of, bias):
            totals = []
            for s in range(size):
                sent = (hidden_of(s), first_of(s), bias)
                sent = [v.astype(BF16) for v in sent]
                if s:
                    sent = [swap(v, axes, size, s) for v in sent]
                totals.append([v.astype(F32) for v in sent])
            return [tree_sum(list(group)) for group in zip(*totals)]

        hidden_grad, first_grad, bias_sum = exchange(
            "c",
            nc,
            lambda s: part(hidden_grad, c ^ s, nc, 0),
            lambda s: part(first_grad, c ^ s, nc, 0),
            bias_sum,
        )
        whole_hidden, whole_first = hidden_grad, first_grad
        hidden_grad, first_grad, bias_sum = exchange(
            ("x", "y"),
            nxy,
            lambda s: part(whole_hidden, x ^ (s // ny), nx, 0)[
                :, (s % ny) * kw : (s % ny + 1) * kw
            ],
            lambda s: part(part(whole_first, x ^ (s // ny), nx, 0), y ^ (s % ny), ny, 1),
            bias_sum,
        )
        half_hidden, half_first = hidden_grad, first_grad
        hidden_grad, first_grad, bias_sum = exchange(
            "z",
            nz,
            lambda s: part(half_hidden, z ^ s, nz, 0),
            lambda s: part(half_first, z ^ s, nz, 0),
            bias_sum,
        )

        def spread(value, axes, size, me, axis):
            return place([value] + [swap(value, axes, size, s) for s in range(1, size)], me, axis)

        hidden_out = hidden_grad.astype(BF16)
        first_out = first_grad.astype(BF16)
        hidden_out = spread(hidden_out, "z", nz, z, 0)
        first_out = spread(first_out, "z", nz, z, 0)
        hidden_out = spread(hidden_out, "x", nx, x, 0)
        first_out = spread(first_out, "x", nx, x, 0)
        first_out = spread(first_out, "y", ny, y, 1)
        hidden_out = spread(hidden_out, "c", nc, c, 0)
        first_out = spread(first_out, "c", nc, c, 0)
        return (
            first_out.astype(F32),
            bias_sum[ny:].reshape(-1),
            hidden_out.astype(F32),
            bias_sum[y],
            decoder_grad,
        )

    return on_device


def solution(mesh):
    dp, mp = mesh.shape["dp"], mesh.shape["mp"]
    nc = 2 if dp % 2 == 0 else 1
    nx = 2 if dp % (2 * nc) == 0 else 1
    nz = dp // (nc * nx)
    fine = Mesh(mesh.devices.reshape(nz, nx, nc, mp), ("z", "x", "c", "y"))
    dps = ("z", "x", "c")
    every = dps + ("y",)
    placed = (
        P(),
        P(),
        P(None, every),
        P(None, every, None),
        P(),
        P(),
        P(None, "y"),
        P("y"),
        P(every, None),
    )
    pieces = nc * nx * nz

    def step(*args):
        window, weight, part_weight = args[1], args[4], args[6]
        rank, hidden = weight.shape
        packed = nc == nx == mp == 2 and window.shape[0] % nc == 0
        packed = packed and rank % (8 * pieces) == 0 and hidden % (16 * pieces) == 0
        packed = packed and part_weight.shape[1] % 128 == 0
        build = make_fast_step if packed else make_step
        return build(nz, nx, nc, mp)(*args)

    return jax.shard_map(
        step,
        mesh=fine,
        in_specs=placed,
        out_specs=(P(), P(), P(None, "y"), P("y"), P(every, None)),
        check_vma=False,
    )
```

```python
import functools

import jax
import jax.numpy as jnp
from jax import lax
from jax.experimental import pallas as pl
from jax.experimental.pallas import tpu as pltpu
from jax.sharding import Mesh, PartitionSpec as P

F32 = jnp.float32
BF16 = jnp.bfloat16


def dot(a, b, contract):
    return lax.dot_general(a, b, (contract, ((), ())), preferred_element_type=F32)


def swap(value, axes, size, step):
    return lax.ppermute(value, axes, [(j, j ^ step) for j in range(size)])


def tree_sum(parts):
    while len(parts) > 1:
        parts = [parts[i] + parts[i + 1] for i in range(0, len(parts), 2)]
    return parts[0]


def place(pieces, me, axis):
    width = pieces[0].shape[axis]
    shape = list(pieces[0].shape)
    shape[axis] *= len(pieces)
    whole = jnp.zeros(shape, pieces[0].dtype)
    for step, piece in enumerate(pieces):
        whole = lax.dynamic_update_slice_in_dim(whole, piece, (me ^ step) * width, axis)
    return whole


def part(value, index, count, axis):
    width = value.shape[axis] // count
    return lax.dynamic_slice_in_dim(value, index * width, width, axis)


VMEM = pl.BlockSpec(memory_space=pltpu.VMEM)
SMEM = pl.BlockSpec(memory_space=pltpu.SMEM)
ANY = pl.BlockSpec(memory_space=pltpu.HBM)


COST_UNIT = 1 << 30


def aligned(index, size):
    return pl.ds(pl.multiple_of(index * size, size), size)


def local_call(body, outs, args, **options):
    return kernel_call(body, outs, args, **options)


def kernel_call(
    body, outs, args, specs=None, out_specs=None, scratch=(), aliases=None, limit=24 << 20, cost=1.0
):
    return pl.pallas_call(
        body,
        out_shape=[jax.ShapeDtypeStruct(shape, kind) for shape, kind in outs],
        in_specs=[VMEM] * len(args) if specs is None else specs,
        out_specs=[VMEM] * len(outs) if out_specs is None else out_specs,
        input_output_aliases=aliases or {},
        scratch_shapes=list(scratch),
        compiler_params=pltpu.CompilerParams(vmem_limit_bytes=limit),
        cost_estimate=pl.CostEstimate(
            flops=int(cost * COST_UNIT), bytes_accessed=1 << 20, transcendentals=0
        ),
    )(*args)


def make_fast_step(nz, nx, nc, ny):
    nxy = nx * ny

    def on_device(
        inputs_store,
        window,
        targets_store,
        jac_store,
        first_weight,
        first_bias,
        hidden_weight,
        hidden_bias,
        decoder_weight,
    ):
        rank, hidden = first_weight.shape
        kw = hidden_weight.shape[1]
        outs, depth = decoder_weight.shape[0], inputs_store.shape[0]
        count = window.shape[0] // nc
        total = (count + 1) * rank
        hrow_c, frow_c = hidden // nc, rank // nc
        hrow_x = hrow_c // nx
        hrow_z, frow_z = hrow_x // nz, frow_c // nz
        brow, lead = 8, 16

        def swaps(values, axes, size):
            moved = [values[0]]
            for step in range(1, size):
                moved.append(swap(values[step], axes, size, step))
            return moved

        shared = hrow_c // 2
        near_rows = shared // nx
        c, x = lax.axis_index("c"), lax.axis_index("x")
        near = lax.dynamic_slice_in_dim(hidden_weight, c * hrow_c + x * near_rows, near_rows)

        def hand_on(in_ref, out_ref):
            out_ref[...] = in_ref[...]

        (near,) = local_call(hand_on, [((near_rows, kw), BF16)], (near,), cost=20, limit=4 << 20)
        rest = lax.dynamic_slice_in_dim(
            hidden_weight, c * hrow_c + shared - lead, hrow_c - shared + lead
        )
        line = lax.broadcasted_iota(jnp.int32, rest.shape, 0)
        rest = jnp.where(line < lead, hidden_bias[None, :], rest)
        _, near_got = swaps([near] * ny, "y", ny)
        _, rest_got = swaps([rest] * ny, "y", ny)
        _, decoder_got = swaps([decoder_weight] * nc, "c", nc)
        _, far_got = swaps([near_got] * nx, "x", nx)
        _, near_core = swaps([near_got] * nc, "c", nc)

        def gather(
            window_ref, jac_ref, target_ref, input_ref, weight_ref, bias_ref,
            own_ref, away_ref, act_ref, turned_ref, sems,
        ):
            me = lax.axis_index("c")
            copies = []
            for u, ref in enumerate((away_ref, own_ref)):
                for i in range(count):
                    row = window_ref[(me ^ u ^ 1) * count + i]
                    copies.append(pltpu.make_async_copy(jac_ref.at[row], ref.at[i], sems.at[u, i]))
            for copy in copies:
                copy.start()
            padded_rows = -(-count // 16) * 16
            line = lax.broadcasted_iota(jnp.int32, (padded_rows, depth), 0)
            place_of = lax.broadcasted_iota(jnp.int32, (padded_rows, depth), 1)
            pad = jnp.zeros((rank - padded_rows, rank), F32)

            def pick(member, table):
                index = jnp.full((padded_rows, depth), -1, jnp.int32)
                for i in range(count):
                    index = jnp.where(line == i, window_ref[member * count + i], index)
                chosen = jnp.where(index == place_of, 1.0, 0.0).astype(BF16)
                return jnp.dot(chosen, table, preferred_element_type=F32)

            inputs = pick(me, input_ref[...])
            turned_ref[...] = jnp.concatenate([inputs, pad]).T
            first_pre = jnp.dot(
                inputs.astype(BF16), weight_ref[...], preferred_element_type=F32
            )[:count]
            act_ref[...] = jnp.tanh(first_pre + bias_ref[...].astype(F32).reshape(1, hidden))
            for member, ref in ((me, own_ref), (me ^ 1, away_ref)):
                target = jnp.concatenate([pick(member, target_ref[...]), pad])
                ref[count] = target.T.astype(BF16)
            for copy in copies:
                copy.wait()

        jac_shape = ((count + 1,) + jac_store.shape[1:], BF16)
        jac_own, jac_away, first_act, turned = local_call(
            gather,
            [jac_shape, jac_shape, ((count, hidden), F32), ((rank, rank), F32)],
            (window, jac_store, targets_store, inputs_store, first_weight, first_bias),
            cost=4,
            specs=[SMEM, ANY, VMEM, VMEM, VMEM, VMEM],
            scratch=[pltpu.SemaphoreType.DMA((nc, count))],
            limit=50 << 20,
        )
        _, jac_got = swaps([jac_away] * nc, "c", nc)

        def warm(act_ref, weight_ref, half_ref, tan_ref, side_ref, lin_ref):
            act = act_ref[...]
            slope = 1.0 - act * act
            weight = weight_ref[...].astype(F32)
            pad = jnp.zeros((rank - count, hidden), F32)
            for s in range(count):
                rows = slice(s * rank, (s + 1) * rank)
                tan_ref[rows] = (slope[s : s + 1] * weight).astype(BF16)
            padded = jnp.concatenate([act, pad])
            tan_ref[count * rank :] = padded.astype(BF16)
            lin_ref[...] = jnp.dot(tan_ref[...], half_ref[...], preferred_element_type=F32)
            slope_side = jnp.concatenate([slope, pad]).T
            weight_side = weight.T
            for s in range(count):
                columns = slice(s * rank, (s + 1) * rank)
                side_ref[:, columns] = (slope_side[:, s : s + 1] * weight_side).astype(BF16)
            side_ref[:, count * rank :] = padded.T.astype(BF16)

        first_tan, first_side, lin_own = local_call(
            warm,
            [((total, hidden), BF16), ((hidden, total), BF16), ((total, kw), F32)],
            (first_act, first_weight, hidden_weight),
            cost=2,
            limit=30 << 20,
        )

        def ready(
            lin_ref, bias_ref, dec_ref, dec_got_ref, jac_ref, jac_got_ref,
            wide_ref, tan_ref, net_ref,
        ):
            my = lax.axis_index("y")
            for b in range(ny):
                columns = slice(b * kw, (b + 1) * kw)
                wide_ref[:outs, columns] = dec_ref[:, aligned(my ^ b, kw)]
                wide_ref[outs:, columns] = dec_got_ref[:, aligned(my ^ b, kw)]
            hidden_tangents(lin_ref, *hidden_slopes(lin_ref, hidden_row(bias_ref)), tan_ref)
            net_ref[...] = dot(wide_ref[:, :kw], tan_ref[...], ((1,), (1,)))
            for s in range(count + 1):
                columns = slice(s * rank, (s + 1) * rank)
                net_ref[:outs, columns] -= jac_ref[s].astype(F32)
                net_ref[outs:, columns] -= jac_got_ref[s].astype(F32)

        def hidden_row(bias_ref):
            return bias_ref[...].astype(F32).reshape(1, kw)

        def hidden_slopes(lin_ref, bias):
            act = jnp.tanh(lin_ref[count * rank : count * rank + count] + bias)
            return act, 1.0 - act * act

        def hidden_tangents(lin_ref, act, slope, tan_ref):
            pad = jnp.zeros((rank - count, kw), F32)
            for s in range(count):
                rows = slice(s * rank, (s + 1) * rank)
                tan_ref[rows] = (slope[s : s + 1] * lin_ref[rows]).astype(BF16)
            tan_ref[count * rank :] = jnp.concatenate([act, pad]).astype(BF16)

        wide, tan_own, net_own = local_call(
            ready,
            [((nc * outs, hidden), BF16), ((total, kw), BF16), ((nc * outs, total), F32)],
            (lin_own, hidden_bias, decoder_weight, decoder_got, jac_own, jac_got),
            cost=1.5,
            limit=16 << 20,
        )
        rest_got, far_got, tan_own = lax.optimization_barrier((rest_got, far_got, tan_own))
        fetched = (near_got, far_got, rest_got, near_core)
        fetched += tuple(swap(value, "c", nc, 1) for value in (far_got, rest_got))

        def main(
            tan1_ref, side_ref, lin_ref, near_ref, far_ref, rest_ref, near2_ref, far2_ref, rest2_ref,
            bias_ref, wide_ref, net_own_ref,
            half_ref, tan_ref, miss_ref, round_ref, sum_ref, out_ref,
            lin_got_ref, back_ref,
        ):
            me, mx = lax.axis_index("c"), lax.axis_index("x")
            for u, refs in enumerate(((near_ref, far_ref, rest_ref), (near2_ref, far2_ref, rest2_ref))):
                base = (me ^ u) * hrow_c
                for a in range(nx):
                    start = pl.multiple_of(base + (mx ^ a) * near_rows, near_rows)
                    half_ref[pl.ds(start, near_rows)] = refs[a][...]
                start = pl.multiple_of(base + shared, shared)
                half_ref[pl.ds(start, hrow_c - shared)] = refs[2][lead:]
            lin_got_ref[...] = jnp.dot(tan1_ref[...], half_ref[...], preferred_element_type=F32)
            bias_got = rest_ref[:lead].astype(F32)[:1]
            own, other = hidden_slopes(lin_ref, hidden_row(bias_ref)), hidden_slopes(lin_got_ref, bias_got)
            hidden_tangents(lin_got_ref, *other, tan_ref)
            net = net_own_ref[...] + dot(wide_ref[:, kw:], tan_ref[...], ((1,), (1,)))
            miss_ref[...] = net.astype(BF16)
            back_ref[...] = dot(miss_ref[...], wide_ref[...], ((0,), (0,)))
            pad = jnp.zeros((rank - count, kw), F32)
            for b, (lin, (act, slope)) in enumerate(((lin_ref, own), (lin_got_ref, other))):
                columns = slice(b * kw, (b + 1) * kw)
                sums = []
                for s in range(count):
                    rows = slice(s * rank, (s + 1) * rank)
                    back = back_ref[rows, columns]
                    sums.append(jnp.sum(back * lin[rows], axis=0, keepdims=True))
                    round_ref[rows, columns] = (back * slope[s : s + 1]).astype(BF16)
                act_back = back_ref[count * rank : count * rank + count, columns]
                pre_back = act_back * slope - 2.0 * act * slope * jnp.concatenate(sums)
                round_ref[count * rank :, columns] = jnp.concatenate([pre_back, pad]).astype(BF16)
                sum_ref[:, columns] = jnp.sum(pre_back, axis=0, keepdims=True)
            out_ref[...] = jnp.dot(
                side_ref[aligned(me ^ 1, hrow_c)], round_ref[:, kw:], preferred_element_type=F32
            ).astype(BF16)

        half_got, tan_got, miss, lin_round, hidden_sum, g_away = local_call(
            main,
            [
                ((hidden, kw), BF16),
                ((total, kw), BF16),
                ((nc * outs, total), BF16),
                ((total, hidden), BF16),
                ((1, hidden), F32),
                ((hrow_c, kw), BF16),
            ],
            (first_tan, first_side, lin_own, *fetched, hidden_bias, wide, net_own),
            cost=5,
            scratch=[pltpu.VMEM((total, kw), F32), pltpu.VMEM((total, hidden), F32)],
            limit=36 << 20,
        )
        _, g_got = swaps([g_away] * nc, "c", nc)

        def between(side_ref, round_ref, own_ref, away_ref):
            me = lax.axis_index("c")
            own_ref[...] = jnp.dot(
                side_ref[aligned(me, hrow_c)], round_ref[:, kw:], preferred_element_type=F32
            )
            away_ref[...] = jnp.dot(
                side_ref[aligned(me ^ 1, hrow_c)], round_ref[:, :kw], preferred_element_type=F32
            ).astype(BF16)

        g_own, g_away = local_call(
            between,
            [((hrow_c, kw), F32), ((hrow_c, kw), BF16)],
            (first_side, lin_round),
            cost=1.5,
            limit=16 << 20,
        )
        _, g_got_last = swaps([g_away] * nc, "c", nc)

        def merge_core(g_ref, got_ref, *out_refs):
            mx = lax.axis_index("x")
            for a, out_ref in enumerate(out_refs):
                rows = aligned(mx ^ a, hrow_x)
                out_ref[...] = (g_ref[rows] + got_ref[rows].astype(F32)).astype(BF16)

        rows_shape = ((hrow_x, kw), BF16)
        plane1, plane3 = local_call(merge_core, [rows_shape] * nx, (g_own, g_got))

        def finish_core(side_ref, round_ref, got_ref, *refs):
            me, g_ref = lax.axis_index("c"), refs[-1]
            g_ref[...] = jnp.dot(
                side_ref[aligned(me, hrow_c)], round_ref[:, :kw], preferred_element_type=F32
            )
            merge_core(g_ref, got_ref, *refs[:-1])

        plane0, plane2 = local_call(
            finish_core,
            [rows_shape] * nx,
            (first_side, lin_round, g_got_last),
            scratch=[pltpu.VMEM((hrow_c, kw), F32)],
            limit=16 << 20,
        )
        plane = [plane0, plane1, plane2, plane3]
        (lin_round, miss, tan_got), _ = lax.optimization_barrier(
            ((lin_round, miss, tan_got), plane[0])
        )
        plane = swaps(plane, ("x", "y"), nxy)

        def lower(
            round_ref, half_ref, got_ref, act_ref, weight_ref, turned_ref, sum_ref,
            own_ref, away_ref, bias_ref, low_ref, first_ref,
        ):
            me, my = lax.axis_index("c"), lax.axis_index("y")
            low_ref[...] = dot(round_ref[:, :kw], half_ref[...], ((1,), (1,)))
            low_ref[...] += dot(round_ref[:, kw:], got_ref[...], ((1,), (1,)))
            act = act_ref[...]
            slope = 1.0 - act * act
            weight = weight_ref[...].astype(F32)
            sums = []
            for s in range(count):
                low = low_ref[s * rank : (s + 1) * rank]
                sums.append(jnp.sum(low * weight, axis=0, keepdims=True))
            act_lower = low_ref[count * rank : count * rank + count]
            pre_lower = act_lower * slope - 2.0 * act * slope * jnp.concatenate(sums)
            turned = turned_ref[...]
            value = jnp.zeros((rank, hidden), F32)
            for s in range(count):
                low = low_ref[s * rank : (s + 1) * rank]
                value = value + low * slope[s : s + 1]
                value = value + turned[:, s : s + 1] * pre_lower[s : s + 1]
            first_ref[...] = value
            own_ref[...] = first_ref[aligned(me, frow_c)]
            away = first_ref[aligned(me ^ 1, frow_c)].astype(BF16)
            for b in range(ny):
                away_ref[b * frow_c : (b + 1) * frow_c] = away[:, b * kw : (b + 1) * kw]
            sums = sum_ref[...]
            halves = [sums[:, :kw], sums[:, kw:]]
            first_sum = jnp.sum(pre_lower, axis=0, keepdims=True)
            bias = jnp.concatenate(
                [
                    jnp.where(my == 0, halves[0], halves[1]),
                    jnp.where(my == 0, halves[1], halves[0]),
                    first_sum[:, :kw],
                    first_sum[:, kw:],
                    jnp.zeros((brow - 2 * ny, kw), F32),
                ]
            ).astype(BF16)
            away_ref[ny * frow_c :] = bias
            bias_ref[...] = bias

        f_own, f_away, b_own = local_call(
            lower,
            [
                ((frow_c, hidden), F32),
                ((ny * frow_c + brow, kw), BF16),
                ((brow, kw), BF16),
            ],
            (lin_round, hidden_weight, half_got, first_act, first_weight, turned, hidden_sum),
            cost=3,
            scratch=[pltpu.VMEM((total, hidden), F32), pltpu.VMEM((rank, hidden), F32)],
            limit=30 << 20,
        )
        _, f_got = swaps([f_away] * nc, "c", nc)

        def merge_first(f_ref, got_ref, b_ref, *out_refs):
            mz = lax.axis_index("z")
            bias = (b_ref[...].astype(F32) + got_ref[ny * frow_c :].astype(F32)).astype(BF16)
            for s, out_ref in enumerate(out_refs):
                rows = aligned(mz ^ s, frow_z)
                for b in range(ny):
                    there = pl.ds(pl.multiple_of(b * frow_c + (mz ^ s) * frow_z, frow_z), frow_z)
                    value = f_ref[rows, b * kw : (b + 1) * kw] + got_ref[there].astype(F32)
                    out_ref[b * frow_z : (b + 1) * frow_z] = value.astype(BF16)
                out_ref[ny * frow_z :] = bias

        side = local_call(
            merge_first, [((ny * frow_z + brow, kw), BF16)] * nz, (f_own, f_got, b_own)
        )
        side = swaps(side, "z", nz)

        def readout(miss_ref, tan_ref, tan_got_ref, own_ref, away_ref):
            for ref, rows in ((own_ref, slice(0, outs)), (away_ref, slice(outs, None))):
                for b, tan in enumerate((tan_ref, tan_got_ref)):
                    ref[:, b * kw : (b + 1) * kw] = jnp.dot(
                        miss_ref[rows], tan[...], preferred_element_type=F32
                    )

        d_own, d_away = local_call(
            readout, [((outs, hidden), F32)] * 2, (miss, tan_own, tan_got), cost=1, limit=16 << 20
        )
        *plane, d_away = lax.optimization_barrier((*plane, d_away))
        d_got = swap(d_away, "c", nc, 1)

        def join(own_ref, got_ref, out_ref):
            my = lax.axis_index("y")
            for b in range(ny):
                columns = slice(b * kw, (b + 1) * kw)
                out_ref[:, aligned(my ^ b, kw)] = own_ref[:, columns] + got_ref[:, columns]

        (decoder_grad,) = local_call(
            join, [((outs, hidden), F32)], (d_own, d_got), cost=1, limit=8 << 20
        )

        def merge_plane(*refs):
            in_refs, out_refs, total_ref = refs[:nxy], refs[nxy:-1], refs[-1]
            mz = lax.axis_index("z")
            total_ref[...] = tree_sum([ref[...].astype(F32) for ref in in_refs])
            for s, out_ref in enumerate(out_refs):
                out_ref[...] = total_ref[aligned(mz ^ s, hrow_z)].astype(BF16)

        line = local_call(
            merge_plane,
            [((hrow_z, kw), BF16)] * nz,
            tuple(plane),
            scratch=[pltpu.VMEM((hrow_x, kw), F32)],
        )
        line = swaps(line, "z", nz)

        def add_rounded(*refs):
            total_sum = tree_sum([ref[...].astype(F32) for ref in refs[:-1]])
            refs[-1][...] = total_sum.astype(BF16)

        (side_sum,) = local_call(add_rounded, [((ny * frow_z + brow, kw), BF16)], tuple(side))
        side = swaps([side_sum] * nxy, ("x", "y"), nxy)
        *line, decoder_grad = lax.optimization_barrier((*line, decoder_grad))
        (piece,) = local_call(add_rounded, [((hrow_z, kw), BF16)], tuple(line))
        pieces = swaps([piece] * nz, "z", nz)

        def finish_side(*refs):
            in_refs, (out_ref, hidden_ref, first_ref) = refs[:nxy], refs[nxy:]
            my = lax.axis_index("y")
            total_sum = tree_sum([ref[...].astype(F32) for ref in in_refs])
            out_ref[...] = total_sum[: ny * frow_z].astype(BF16)
            bias = total_sum[ny * frow_z :]
            hidden_ref[...] = jnp.where(my == 0, bias[0:1], bias[1:2]).reshape(kw)
            for b in range(ny):
                row = bias[ny + b : ny + b + 1]
                first_ref[b * kw : (b + 1) * kw] = row.reshape(kw)

        side_piece, hidden_bias_out, first_bias_out = local_call(
            finish_side, [((ny * frow_z, kw), BF16), ((kw,), F32), ((hidden,), F32)], tuple(side)
        )
        side_pieces = swaps([side_piece] * nz, "z", nz)

        def stack(*refs):
            mz = lax.axis_index("z")
            for s, ref in enumerate(refs[:nz]):
                refs[nz][mz ^ s] = ref[...]

        (both,) = local_call(stack, [((nz, hrow_z, kw), BF16)], tuple(pieces))
        (first,) = local_call(stack, [((nz, ny * frow_z, kw), BF16)], tuple(side_pieces))
        _, across = swaps([both] * nx, "x", nx)
        _, both_core = swaps([both] * nc, "c", nc)
        _, first_core = swaps([first] * nc, "c", nc)
        _, across_core = swaps([across] * nc, "c", nc)

        def put(refs, base, size, out_ref, stage_ref, sem_ref, slot):
            copies = []
            for i in range(nz):
                stage_ref[slot * nz + i] = refs[i].astype(F32)
                copies.append(
                    pltpu.make_async_copy(
                        stage_ref.at[slot * nz + i],
                        out_ref.at[aligned(base * nz + i, size)],
                        sem_ref.at[slot * nz + i],
                    )
                )
                copies[-1].start()
            return copies

        def early(both_ref, core_ref, out_ref, stage_ref, sem_ref):
            mx, mc = lax.axis_index("x"), lax.axis_index("c")
            copies = put(both_ref, mc * nx + mx, hrow_z, out_ref, stage_ref, sem_ref, 0)
            copies += put(core_ref, (mc ^ 1) * nx + mx, hrow_z, out_ref, stage_ref, sem_ref, 1)
            for copy in copies:
                copy.wait()

        stage = [pltpu.VMEM((nc * nz, hrow_z, kw), F32), pltpu.SemaphoreType.DMA((nc * nz,))]

        def top(own_ref, core_ref, first_ref):
            mc = lax.axis_index("c")
            for u, ref in enumerate((own_ref, core_ref)):
                for i in range(nz):
                    rows = aligned((mc ^ u) * nz + i, frow_z)
                    value = ref[i].astype(F32)
                    for b in range(ny):
                        first_ref[rows, b * kw : (b + 1) * kw] = value[b * frow_z : (b + 1) * frow_z]

        def late(core, held_ref, across_ref, out_ref, stage_ref, sem_ref):
            mx, mc = lax.axis_index("x"), lax.axis_index("c")
            base = (mc ^ core) * nx + (mx ^ 1)
            for copy in put(across_ref, base, hrow_z, out_ref, stage_ref, sem_ref, 0):
                copy.wait()

        (hidden_out,) = local_call(
            early,
            [((hidden, kw), F32)],
            (both, both_core),
            out_specs=[ANY],
            scratch=stage,
            limit=8 << 20,
        )
        (first_out,) = local_call(top, [((rank, hidden), F32)], (first, first_core), limit=4 << 20)
        for core, value in ((0, across), (1, across_core)):
            (hidden_out,) = local_call(
                functools.partial(late, core),
                [((hidden, kw), F32)],
                (hidden_out, value),
                specs=[ANY, VMEM],
                out_specs=[ANY],
                scratch=stage,
                aliases={0: 0},
                limit=8 << 20,
            )
        return (first_out, first_bias_out, hidden_out, hidden_bias_out, decoder_grad)

    return on_device


def make_step(nz, nx, nc, ny):
    nxy = nx * ny

    def on_device(
        inputs_store,
        window,
        targets_store,
        jac_store,
        first_weight,
        first_bias,
        hidden_weight,
        hidden_bias,
        decoder_weight,
    ):
        z, x, c, y = (lax.axis_index(name) for name in ("z", "x", "c", "y"))
        rank, hidden = first_weight.shape
        kw = hidden_weight.shape[1]
        pieces = [hidden_weight]
        biases = [hidden_bias]
        mine = part(hidden_weight, c, nc, 0)
        for t in range(1, ny):
            got = swap(mine, "y", ny, t)
            rest = [got] + [swap(got, "c", nc, u) for u in range(1, nc)]
            pieces.append(place(rest, c, 0))
            biases.append(swap(hidden_bias, "y", ny, t))
        wide_hidden = jnp.concatenate(pieces, axis=1)
        wide_bias = jnp.concatenate(biases)
        jac_parts, target_parts, decoder_parts = [], [], []
        for u in range(nc):
            rows = part(window, c ^ u, nc, 0)
            jac, target = jac_store[rows], targets_store[rows]
            decoder = decoder_weight
            if u:
                jac, target, decoder = (swap(v, "c", nc, u) for v in (jac, target, decoder))
            jac_parts.append(jac)
            target_parts.append(target)
            decoder_parts.append(decoder)
        jac = jnp.concatenate(jac_parts, axis=1)
        target = jnp.concatenate(target_parts, axis=1)
        decoder = jnp.concatenate(decoder_parts, axis=0)
        decoder = jnp.concatenate([part(decoder, y ^ t, ny, 1) for t in range(ny)], axis=1)
        inputs = inputs_store[part(window, c, nc, 0)]
        count = inputs.shape[0]
        weight_one = first_weight.astype(F32)
        first_act = jnp.tanh(dot(inputs, first_weight, ((1,), (0,))) + first_bias.astype(F32))
        first_slope = 1.0 - first_act * first_act
        first_tan = (first_slope[:, None, :] * weight_one[None]).astype(BF16)
        first_tan = first_tan.reshape(count * rank, hidden)
        first_round = first_act.astype(BF16)
        hidden_lin = dot(first_tan, wide_hidden, ((1,), (0,))).reshape(count, rank, -1)
        hidden_act = jnp.tanh(
            dot(first_round, wide_hidden, ((1,), (0,))) + wide_bias.astype(F32)
        )
        hidden_slope = 1.0 - hidden_act * hidden_act
        hidden_tan = (hidden_slope[:, None, :] * hidden_lin).astype(BF16)
        hidden_round = hidden_act.astype(BF16)
        output_miss = dot(hidden_round, decoder, ((1,), (1,))) - target.astype(F32)
        output_miss = output_miss.astype(BF16)
        jac_net = dot(decoder, hidden_tan, ((1,), (2,)))
        jac_miss = (jac_net - jac.transpose(1, 0, 2).astype(F32)).astype(BF16)
        jac_miss = jac_miss.reshape(-1, count * rank)
        grad = dot(output_miss, hidden_round, ((0,), (0,))) + dot(
            jac_miss, hidden_tan.reshape(count * rank, -1), ((1,), (0,))
        )
        blocks = jnp.split(grad, nc, axis=0)
        own = [blocks[0]] + [swap(blocks[u], "c", nc, u) for u in range(1, nc)]
        grad = tree_sum(own)
        decoder_grad = place(jnp.split(grad, ny, axis=1), y, 1)

        act_back = dot(output_miss, decoder, ((1,), (0,)))
        tan_back = dot(jac_miss, decoder, ((0,), (0,))).reshape(count, rank, -1)
        pre_back = act_back * hidden_slope - 2.0 * hidden_act * hidden_slope * jnp.sum(
            tan_back * hidden_lin, axis=1
        )
        lin_round = (tan_back * hidden_slope[:, None, :]).astype(BF16)
        lin_round = lin_round.reshape(count * rank, -1)
        pre_round = pre_back.astype(BF16)
        hidden_grad = dot(first_round, pre_round, ((0,), (0,))) + dot(
            first_tan, lin_round, ((0,), (0,))
        )
        tan_lower = dot(lin_round, wide_hidden, ((1,), (1,))).reshape(count, rank, hidden)
        act_lower = dot(pre_round, wide_hidden, ((1,), (1,)))
        pre_lower = act_lower * first_slope - 2.0 * first_act * first_slope * jnp.sum(
            tan_lower * weight_one[None], axis=1
        )
        first_grad = jnp.einsum(
            "sr,sh->rh", inputs.astype(F32), pre_lower, precision=lax.Precision.HIGHEST
        ) + jnp.sum(tan_lower * first_slope[:, None, :], axis=0)
        hidden_bsum = jnp.sum(pre_back, axis=0).reshape(ny, kw)
        hidden_bsum = place([hidden_bsum[t : t + 1] for t in range(ny)], y, 0)
        first_bsum = jnp.sum(pre_lower, axis=0).reshape(ny, kw)
        bias_sum = jnp.concatenate([hidden_bsum, first_bsum])

        def exchange(axes, size, hidden_of, first_of, bias):
            totals = []
            for s in range(size):
                sent = (hidden_of(s), first_of(s), bias)
                sent = [v.astype(BF16) for v in sent]
                if s:
                    sent = [swap(v, axes, size, s) for v in sent]
                totals.append([v.astype(F32) for v in sent])
            return [tree_sum(list(group)) for group in zip(*totals)]

        hidden_grad, first_grad, bias_sum = exchange(
            "c",
            nc,
            lambda s: part(hidden_grad, c ^ s, nc, 0),
            lambda s: part(first_grad, c ^ s, nc, 0),
            bias_sum,
        )
        whole_hidden, whole_first = hidden_grad, first_grad
        hidden_grad, first_grad, bias_sum = exchange(
            ("x", "y"),
            nxy,
            lambda s: part(whole_hidden, x ^ (s // ny), nx, 0)[
                :, (s % ny) * kw : (s % ny + 1) * kw
            ],
            lambda s: part(part(whole_first, x ^ (s // ny), nx, 0), y ^ (s % ny), ny, 1),
            bias_sum,
        )
        half_hidden, half_first = hidden_grad, first_grad
        hidden_grad, first_grad, bias_sum = exchange(
            "z",
            nz,
            lambda s: part(half_hidden, z ^ s, nz, 0),
            lambda s: part(half_first, z ^ s, nz, 0),
            bias_sum,
        )

        def spread(value, axes, size, me, axis):
            return place([value] + [swap(value, axes, size, s) for s in range(1, size)], me, axis)

        hidden_out = hidden_grad.astype(BF16)
        first_out = first_grad.astype(BF16)
        hidden_out = spread(hidden_out, "z", nz, z, 0)
        first_out = spread(first_out, "z", nz, z, 0)
        hidden_out = spread(hidden_out, "x", nx, x, 0)
        first_out = spread(first_out, "x", nx, x, 0)
        first_out = spread(first_out, "y", ny, y, 1)
        hidden_out = spread(hidden_out, "c", nc, c, 0)
        first_out = spread(first_out, "c", nc, c, 0)
        return (
            first_out.astype(F32),
            bias_sum[ny:].reshape(-1),
            hidden_out.astype(F32),
            bias_sum[y],
            decoder_grad,
        )

    return on_device


def solution(mesh):
    dp, mp = mesh.shape["dp"], mesh.shape["mp"]
    nc = 2 if dp % 2 == 0 else 1
    nx = 2 if dp % (2 * nc) == 0 else 1
    nz = dp // (nc * nx)
    fine = Mesh(mesh.devices.reshape(nz, nx, nc, mp), ("z", "x", "c", "y"))
    dps = ("z", "x", "c")
    every = dps + ("y",)
    placed = (
        P(),
        P(),
        P(None, every),
        P(None, every, None),
        P(),
        P(),
        P(None, "y"),
        P("y"),
        P(every, None),
    )
    pieces = nc * nx * nz

    def step(*args):
        window, weight, part_weight = args[1], args[4], args[6]
        rank, hidden = weight.shape
        packed = nc == nx == mp == 2 and window.shape[0] % nc == 0
        packed = packed and rank % (8 * pieces) == 0 and hidden % (16 * pieces) == 0
        packed = packed and part_weight.shape[1] % 128 == 0
        build = make_fast_step if packed else make_step
        return build(nz, nx, nc, mp)(*args)

    return jax.shard_map(
        step,
        mesh=fine,
        in_specs=placed,
        out_specs=(P(), P(), P(None, "y"), P("y"), P(every, None)),
        check_vma=False,
    )
```
